32 devices in a mesh: row: 4 (over x, core), col: 8 (over z, y).
Axes of the slice: x: 2, y: 2, z: 4, core: 2. Of those that a mesh axis runs over, the one named last changes fastest.
Arguments:
- pooled: bfloat16 [2048, 1152], P(('row', 'col')), may hold values from -32 to 32
- hidden: bfloat16 [2048, 4304], P(('row', 'col')), may hold values from -6 to 6
- text: bfloat16 [2048, 1152], P(('row', 'col')), may hold values from -12 to 12
- weight: float32 [1152, 4304], P('col', 'row'), may hold values from -0.09375 to 0.09375
- row_moment: float32 [1152], P('col'), may hold values from 1e-07 to 1e-05
- col_moment: float32 [4304], P('row'), may hold values from 1e-07 to 1e-05
- log_scale: float32 [], replicated, may hold values from 4.2 to 4.8
- bias: float32 [], replicated, may hold values from -16 to -12
Outputs:
- update: float32 [1152, 4304], P('col', 'row')
- new_row: float32 [1152], P('col')
- new_col: float32 [4304], P('row')
- loss: float32 [], replicated
The draws below stay inside these ranges and needn't reach their ends.
All inputs are finite; a program needn't handle non-finite values.
Results may differ from the reference program's by a relative error of at most 0.004.
Values may be sent and summed in bfloat16 or wider, within the bound.
A program may use at most 128 MiB of HBM per device.

```python
import math
import jax
import jax.numpy as jnp
from jax import lax

D = 1152
FF = 4304
TOK_DEV = 64
BATCH = 2048
N_ROW = 4
N_COL = 8


def noise_block(key, shape):
    return jax.random.normal(key, shape, jnp.float32)


def pair_parts(key):
    folded = jax.random.fold_in(key, 4242)
    subkeys = jax.random.split(folded, 6)
    group_count = 16
    centers = noise_block(subkeys[0], (group_count, D))
    members = jax.random.randint(subkeys[1], (BATCH,), 0, group_count)
    onehot = (members[:, None] == jnp.arange(group_count, dtype=jnp.int32)[None, :]).astype(jnp.float32)
    cluster = jnp.dot(onehot, centers, precision=lax.Precision.HIGHEST)
    shared = noise_block(subkeys[2], (BATCH, D))
    strength = jax.random.uniform(subkeys[3], (BATCH, 1), jnp.float32, 0.1, 0.5)
    own_image = noise_block(subkeys[4], (BATCH, D))
    own_text = noise_block(subkeys[5], (BATCH, D))
    cluster_weight = 0.5
    image_side = cluster_weight * cluster + shared + 1.5 * own_image
    text_side = cluster_weight * cluster + strength * shared + 1.5 * own_text
    return (jnp.clip(image_side, -32.0, 32.0), jnp.clip(text_side, -12.0, 12.0))


def draw_pooled(key, part):
    return pair_parts(key)[0].astype(jnp.bfloat16)


def draw_text(key, part):
    return pair_parts(key)[1].astype(jnp.bfloat16)


def block_levels(key, extent, cuts, least, largest):
    loudness, own = 1.0, jax.random.fold_in(key, 6)
    for axis_at, shards_of in cuts:
        heights = jnp.exp(jax.random.uniform(jax.random.fold_in(own, axis_at), (shards_of,), jnp.float32, least / len(cuts), largest / len(cuts)))
        loudness = loudness * jnp.repeat(heights, extent[axis_at] // shards_of).reshape([-1 if axis == axis_at else 1 for axis in range(len(extent))])
    return loudness


def scatter_about(key, shape, spread, bound, cuts=(), kind=jnp.bfloat16):
    array = jax.random.normal(key, shape, jnp.float32) * spread
    if len(cuts) > 0:
        array = block_levels(key, shape, cuts, -0.22, 0.18) * array
    return jnp.clip(array, min=-bound, max=bound).astype(kind)


def setup_inputs(seed: int = 0) -> dict:
    streams_of = jax.random.split(jax.random.key(seed), 9)
    pooled = draw_pooled(jax.random.fold_in(streams_of[8], 71), 0)
    hidden = scatter_about(streams_of[1], (BATCH, FF), 1.0, 6.0, ((0, 32),))
    text = draw_text(jax.random.fold_in(streams_of[8], 71), 0)
    weight = scatter_about(streams_of[3], (D, FF), FF ** -0.5, 0.09375, ((0, 8), (1, 4)), jnp.float32)
    row_moment = jnp.clip(jnp.exp(math.log(9.999999747378752e-06) - 4.6051701 * jax.random.uniform(streams_of[4], (D,), jnp.float32) ** block_levels(streams_of[4], (D,), ((0, 8),), -0.2, 0.2)), 1.0000000116860974e-07, 9.999999747378752e-06)
    col_moment = jnp.clip(jnp.exp(math.log(9.999999747378752e-06) - 4.6051701 * jax.random.uniform(streams_of[5], (FF,), jnp.float32) ** block_levels(streams_of[5], (FF,), ((0, 4),), -0.2, 0.2)), 1.0000000116860974e-07, 9.999999747378752e-06)
    log_scale = jnp.clip(jax.random.uniform(streams_of[6], (), jnp.float32, 4.2, 4.8), 4.2, 4.8)
    bias = jnp.clip(jax.random.uniform(streams_of[7], (), jnp.float32, -16.0, -12.0), -16.0, -12.0)
    return dict(pooled=pooled, hidden=hidden, text=text, weight=weight, row_moment=row_moment, col_moment=col_moment, log_scale=log_scale, bias=bias)


EPSILON = 1e-06
DECAY_RATE = 0.8
CLIP_LEVEL = 1.0
FLOOR_VALUE = 1e-30

def reference(pooled, hidden, text, weight, row_moment, col_moment, log_scale, bias):
    batch_total = TOK_DEV * N_ROW * N_COL
    weight_half = weight.astype(jnp.bfloat16)
    projected = jnp.dot(hidden, weight_half.T, preferred_element_type=jnp.float32)
    mixed_rows = pooled.astype(jnp.float32) + projected
    length = jnp.sqrt(lax.optimization_barrier(jnp.sum(mixed_rows * mixed_rows, axis=1, keepdims=True)) + EPSILON)
    image_unit = mixed_rows / length
    images = image_unit.astype(jnp.bfloat16)
    text_float = text.astype(jnp.float32)
    text_units = (text_float / jnp.sqrt(lax.optimization_barrier(jnp.sum(text_float * text_float, axis=1, keepdims=True)) + EPSILON)).astype(jnp.bfloat16)
    logit_scale = jnp.exp(log_scale.astype(jnp.float32))
    block_rows = batch_total // N_ROW
    image_blocks = images.reshape(N_ROW, block_rows, D)
    text_ids = jnp.arange(batch_total, dtype=jnp.int32)

    def one_block(block_item):
        image_block, block_index = block_item
        image_ids = block_index * block_rows + jnp.arange(block_rows, dtype=jnp.int32)
        logits = logit_scale * jnp.dot(image_block, text_units.T, preferred_element_type=jnp.float32) + bias
        label_sign = jnp.where(image_ids[:, None] == text_ids[None, :], jnp.float32(1.0), jnp.float32(-1.0))
        loss_sum = jnp.sum(jax.nn.softplus(-label_sign * logits))
        grad_logits = (-label_sign * jax.nn.sigmoid(-label_sign * logits) / batch_total).astype(jnp.bfloat16)
        return (loss_sum, logit_scale * jnp.dot(grad_logits, text_units, preferred_element_type=jnp.float32))
    loss_sums, unit_grads = lax.map(one_block, (image_blocks, jnp.arange(N_ROW, dtype=jnp.int32)))
    loss = jnp.sum(loss_sums) / batch_total
    unit_grad = unit_grads.reshape(batch_total, D)
    mixed_grad = ((unit_grad - image_unit * lax.optimization_barrier(jnp.sum(image_unit * unit_grad, axis=1, keepdims=True))) / length).astype(jnp.bfloat16)
    gradient = jnp.dot(mixed_grad.T, hidden, preferred_element_type=jnp.float32)
    squared = gradient * gradient + FLOOR_VALUE
    new_row = DECAY_RATE * row_moment + (1.0 - DECAY_RATE) * lax.optimization_barrier(jnp.mean(squared, axis=1))
    new_col = DECAY_RATE * col_moment + (1.0 - DECAY_RATE) * lax.optimization_barrier(jnp.mean(squared, axis=0))
    second = new_row[:, None] * new_col[None, :]
    raw_update = gradient / jnp.sqrt(second)
    update_rms = jnp.sqrt(jnp.mean(raw_update * raw_update))
    update = raw_update / jnp.maximum(1.0, update_rms / CLIP_LEVEL)
    return (update, new_row, new_col, loss)
```

```python
import functools

import jax
import jax.numpy as jnp
from jax import lax
from jax.experimental import pallas as pl
from jax.experimental.pallas import tpu as pltpu
from jax.sharding import PartitionSpec as P

EPSILON = 1e-06
DECAY_RATE = 0.8
CLIP_LEVEL = 1.0
FLOOR_VALUE = 1e-30
CORES = 2
LOW = 2
MESH = pl.DeviceIdType.MESH
F32 = jnp.float32
BF16 = jnp.bfloat16


def dot_nt(a, b):
    return lax.dot_general(a, b, (((1,), (1,)), ((), ())), preferred_element_type=F32)


def kernel(
    sizes,
    hid_in, w_in, pool_in, text_in, rm_in, cm_in, ls_ref, bias_ref,
    upd_ref, nr_ref, nc_ref, loss_ref,
    hv, wv, pv, tv, rmv, cmv, hs, pool, rmc,
    hid, wg, txa, part, pre, summed, proj, img_s, img_r, ug_s, ug_r, mg_s, mga, turned, gp, gz_s, gz,
    rsb, csb, stb, ld,
    hid_ss, hid_rs, w_ss, w_rs, tz_ss, tp_ss, t_rs, td_ss, td_rs, pp_ss, pp_rs, p_ss, p_rs, pair_ss, pair_rs,
    mg_ss, mg_rs, g_ss, g_rs, row_ss, row_rs, col_ss, col_rs, st_ss, st_rs,
):
    R, C, X, Z, T, Db, Dp, Fb, chunk, K = sizes
    L = LOW
    plane = R * L
    devices = R * C
    batch = devices * T
    r = lax.axis_index("row")
    c = lax.axis_index("col")
    z, y = c // L, c % L
    x, core = r // CORES, r % CORES
    q = r * L + y
    finish = []
    me = r * C + c
    Dc = Dp // K

    loads = [
        pltpu.make_async_copy(src, dst, ld.at[i])
        for i, (src, dst) in enumerate(
            ((w_in, wv), (hid_in, hv), (text_in, tv), (pool_in, pv), (rm_in, rmv), (cm_in, cmv))
        )
    ]
    for load in loads:
        load.start()
    barrier = pltpu.get_barrier_semaphore()

    def greet(o, _):
        other = lax.rem(me + o, devices)
        pl.semaphore_signal(barrier, inc=1, device_id=(other // C, other % C), device_id_type=MESH)
        return _

    lax.fori_loop(1, devices, greet, 0)

    def send(src, dst, ss, rs, device, cond=None):
        def make():
            return pltpu.make_async_remote_copy(
                src_ref=src, dst_ref=dst, send_sem=ss, recv_sem=rs,
                device_id=device, device_id_type=MESH,
            )

        if cond is None:
            make().start()
            finish.append(lambda: make().wait_send())
        else:
            pl.when(cond)(lambda: make().start())
            finish.append(lambda: pl.when(cond)(lambda: make().wait_send()))

    def arrived(slot, rs):
        pltpu.make_async_copy(slot, slot, rs).wait()

    def plane_peer(o):
        other = lax.rem(q + o, plane)
        return other, other // L, other % L

    def rows(index, count):
        return pl.ds(pl.multiple_of(index * count, count), count)

    def by_half(value, store):
        for h in range(L):
            for k in range(Z):
                at = (k * L + h) * Db
                store(h, k * Dp, value[:, at:at + Db])

    own_slot = x * C + c
    loads[0].wait()
    if Dp != Db:
        wg[rows(z, Dp)] = jnp.zeros((Dp, Fb), BF16)
        txa[:, rows(own_slot, T), :] = jnp.zeros((L, T, Z * Dp), BF16)
        pool[...] = jnp.zeros(pool.shape, F32)
    wg[pl.ds(pl.multiple_of(z * Dp, Dp), Db)] = wv[...].astype(BF16)
    loads[1].wait()
    for k in range(R):
        hs[k] = hv[:, k * Fb:(k + 1) * Fb]
    hid[rows(q, T)] = hs[r]
    loads[2].wait()
    tf = tv[...].astype(F32)
    tn = tf / jnp.sqrt(jnp.sum(tf * tf, axis=1, keepdims=True) + EPSILON)

    def put_text(h, at, value):
        txa[h, rows(own_slot, T), at:at + Db] = value.astype(BF16)

    by_half(tn, put_text)
    pl.semaphore_wait(barrier, devices - 1)
    for o in range(1, plane):
        _, r2, y2 = plane_peer(o)
        send(hs.at[r2], hid.at[rows(q, T)], hid_ss.at[o], hid_rs.at[q], (r2, z * L + y2))

    def text_place(zs):
        return x * C + zs * L + y

    def neighbours():
        along_x = [(lax.rem(x + o, X), y) for o in range(1, X)]
        return along_x + [(x, lax.rem(y + o, L)) for o in range(1, L)]

    def relay(s):
        for d, direction in enumerate((1, -1)):
            if s == 0 and d:
                continue
            zs = z - direction * s
            has = jnp.logical_and(zs >= 0, zs < Z)
            block = jnp.clip(zs, 0, Z - 1)
            for n, (x2, y2) in enumerate(neighbours()):
                place = x2 * C + block * L + y2
                at = txa.at[:, rows(place, T), :]
                if s:
                    pl.when(has)(lambda: arrived(at, t_rs.at[place]))
                else:
                    arrived(at, t_rs.at[place])
                h = 0 if n < X - 1 else 1
                half = txa.at[h, rows(place, T), :]
                onward = neighbours()[X - 1:] if h == 0 else neighbours()[:X - 1]
                for m, (x3, y3) in enumerate(onward):
                    send(
                        half, half, td_ss.at[d, s, n, m], td_rs.at[place, h],
                        (x3 * CORES + core, z * L + y3), has if s else None,
                    )

    for s in range(Z):
        for d, direction in enumerate((1, -1)):
            zs = z - direction * s
            nz = z + direction
            has = jnp.logical_and(zs >= 0, zs < Z)
            go = jnp.logical_and(has, jnp.logical_and(nz >= 0, nz < Z))
            place = text_place(jnp.clip(zs, 0, Z - 1))
            at = txa.at[:, rows(place, T), :]
            if s:
                pl.when(has)(lambda: arrived(at, t_rs.at[place]))
            send(at, at, tz_ss.at[d, s], t_rs.at[place], (r, jnp.clip(nz, 0, Z - 1) * L + y), go)
            if s or d == 0:
                for n, (x2, y2) in enumerate(neighbours()):
                    send(
                        at, at, tp_ss.at[d, s, n], t_rs.at[place],
                        (x2 * CORES + core, z * L + y2), has if s else None,
                    )
        for d, direction in enumerate((1, -1)):
            zs = z - direction * s
            nz = z + direction
            has = jnp.logical_and(zs >= 0, zs < Z)
            go = jnp.logical_and(has, jnp.logical_and(nz >= 0, nz < Z))
            block = jnp.clip(zs, 0, Z - 1)
            at = wg.at[rows(block, Dp)]
            if s:
                pl.when(has)(lambda: arrived(at, w_rs.at[block]))
            send(
                at, at, w_ss.at[d, s], w_rs.at[block],
                (r, jnp.clip(nz, 0, Z - 1) * L + y), go,
            )
        if s:
            relay(s - 1)
        else:
            loads[3].wait()

            def put_pool(h, at, value):
                pool[h, :, at:at + Db] = value

            by_half(pv[...].astype(F32), put_pool)
            loads[4].wait()
            loads[5].wait()
            eye = lax.broadcasted_iota(jnp.int32, (Db, Db), 0) == lax.broadcasted_iota(jnp.int32, (Db, Db), 1)
            line = jnp.broadcast_to(rmv[...].reshape(1, Db), (Db, Db))
            rmc[...] = jnp.sum(jnp.where(eye, line, 0.0), axis=1, keepdims=True)
    for o in range(1, plane):
        other, _, _ = plane_peer(o)
        arrived(hid.at[rows(other, T)], hid_rs.at[other])

    part[...] = dot_nt(hid[...], wg[...])
    partner = (x * CORES + (1 - core), c)
    for o in range(1, X + 1):
        x2 = lax.rem(x + o, X)
        send(
            part.at[rows(x2 * CORES + 1 - core, L * T)], pre.at[x2],
            pp_ss.at[o], pp_rs.at[x2], partner,
        )
    relay(Z - 1)
    for o in range(1, X + 1):
        x2 = lax.rem(x + o, X)
        arrived(pre.at[x2], pp_rs.at[x2])
        summed[x2] = part[rows(x2 * CORES + core, L * T)] + pre[x2]
        for k in range(L):
            y2 = lax.rem(y + 1 + k, L)
            if o == X and k == L - 1:
                proj[x, y] = summed[x, rows(y, T)]
            else:
                send(
                    summed.at[x2, rows(y2, T)], proj.at[x, y], p_ss.at[o * L + k],
                    p_rs.at[x * L + y], (x2 * CORES + core, z * L + y2),
                )
    for o in range(1, X * L):
        other = lax.rem(x * L + y + o, X * L)
        arrived(proj.at[other // L, other % L], p_rs.at[other])
    mixed = []
    for h in range(L):
        total = proj[0, h]
        for k in range(1, X):
            total = total + proj[k, h]
        mixed.append(pool[h] + total)
    square = sum(jnp.sum(m * m, axis=1, keepdims=True) for m in mixed)
    length = jnp.sqrt(square + EPSILON)
    unit = [m / length for m in mixed]
    for h in range(L):
        img_s[h] = unit[h].astype(BF16)
    send(img_s, img_r, pair_ss.at[0], pair_rs.at[0], partner)

    for ox in range(1, X):
        for oy in range(1, L):
            for zs in range(Z):
                place = lax.rem(x + ox, X) * C + zs * L + lax.rem(y + oy, L)
                for h in range(L):
                    arrived(txa.at[h, rows(place, T), :], td_rs.at[place, h])

    scale = jnp.exp(jnp.full((1, 1), ls_ref[0], F32))
    bias = jnp.full((1, 1), bias_ref[0], F32)
    steps = X * C * T // chunk

    def pairs(images, own):
        halves = [images[h] for h in range(L)]

        def step(i, carry):
            loss, grads = carry
            cut = pl.ds(pl.multiple_of(i * chunk, chunk), chunk)
            texts = [txa[h, cut, :] for h in range(L)]
            logits = scale * sum(dot_nt(halves[h], texts[h]) for h in range(L)) + bias
            if own:
                row_id = lax.broadcasted_iota(jnp.int32, logits.shape, 0) + own_slot * T
                col_id = lax.broadcasted_iota(jnp.int32, logits.shape, 1) + i * chunk
                sign = jnp.where(row_id == col_id, F32(1.0), F32(-1.0))
            else:
                sign = F32(-1.0)
            u = -sign * logits
            e = jnp.exp(-jnp.abs(u))
            loss = loss + jnp.sum(jnp.maximum(u, 0.0) + jnp.log1p(e), axis=1, keepdims=True)
            sig = jnp.where(u >= 0, F32(1.0), e) / (1.0 + e)
            pg = (-sign * sig / batch).astype(BF16)
            grads = tuple(
                grads[h] + jnp.dot(pg, texts[h], preferred_element_type=F32) for h in range(L)
            )
            return loss, grads

        zero = (jnp.zeros((T, 1), F32), tuple(jnp.zeros((T, Z * Dp), F32) for _ in range(L)))
        if steps == 1:
            return step(0, zero)
        return lax.fori_loop(0, steps, step, zero)

    arrived(img_r, pair_rs.at[0])
    loss_b, grads_b = pairs(img_r, False)
    for h in range(L):
        ug_s[h] = scale * grads_b[h]
    send(ug_s, ug_r, pair_ss.at[1], pair_rs.at[1], partner)
    loss_a, grads_a = pairs(img_s, True)
    arrived(ug_r, pair_rs.at[1])
    ug = [scale * grads_a[h] + ug_r[h] for h in range(L)]
    inner = sum(jnp.sum(unit[h] * ug[h], axis=1, keepdims=True) for h in range(L))
    for h in range(L):
        mg_s[h] = ((ug[h] - unit[h] * inner) / length).astype(BF16)
    for o in range(1, X * L):
        other = lax.rem(x * L + y + o, X * L)
        send(
            mg_s.at[other % L], mga.at[rows(q, T)], mg_ss.at[o], mg_rs.at[q],
            ((other // L) * CORES + core, z * L + other % L),
        )
    send(mg_s.at[y], mga.at[rows(q, T)], mg_ss.at[0], mg_rs.at[q], partner)
    mga[rows(q, T)] = mg_s[y]
    for o in range(1, X * L):
        other = lax.rem(x * L + y + o, X * L)
        source = ((other // L) * CORES + core) * L + other % L
        at = mga.at[rows(source, T)]
        arrived(at, mg_rs.at[source])
        send(at, at, mg_ss.at[X * L + o], mg_rs.at[source], partner)
    for o in range(X * L):
        other = lax.rem(x * L + y + o, X * L)
        source = ((other // L) * CORES + 1 - core) * L + other % L
        arrived(mga.at[rows(source, T)], mg_rs.at[source])

    turned[...] = mga[...].T

    def own_part(zd):
        gp[zd] = jnp.dot(turned[rows(zd, Dp)], hid[...], preferred_element_type=F32)

    def pieces(tau, d):
        place = z if d == 0 else Z - 1 - z
        i = tau - 2 * place
        zd = jnp.clip(i, 0, Z * K - 1) // K
        k = jnp.clip(i, 0, Z * K - 1) % K
        zd = Z - 1 - zd if d == 0 else zd
        beyond = zd > z if d == 0 else zd < z
        ready = jnp.logical_and(i >= 0, i < Z * K)
        cut = rows(k, Dc)
        copy = pltpu.make_async_remote_copy(
            src_ref=gz_s.at[zd, cut], dst_ref=gz.at[d, zd, cut],
            send_sem=g_ss.at[d, zd, k], recv_sem=g_rs.at[d, zd, k],
            device_id=(r, jnp.clip(z + (1 if d == 0 else -1), 0, Z - 1) * L + y), device_id_type=MESH,
        )
        return place, zd, k, cut, jnp.logical_and(ready, beyond), jnp.logical_and(ready, zd == z), copy

    def step(tau, _):
        for d in range(2):
            place, zd, k, cut, passing, ending, copy = pieces(tau, d)
            at = gz.at[d, zd, cut]

            def first():
                gz_s[zd, cut] = gp[zd, cut].astype(BF16)
                copy.start()

            def onward():
                arrived(at, g_rs.at[d, zd, k])
                gz_s[zd, cut] = (gp[zd, cut] + at[...].astype(F32)).astype(BF16)
                copy.start()

            def last():
                arrived(at, g_rs.at[d, zd, k])
                gp[zd, cut] = gp[zd, cut] + at[...].astype(F32)

            pl.when(jnp.logical_and(passing, place == 0))(first)
            pl.when(jnp.logical_and(passing, place > 0))(onward)
            pl.when(jnp.logical_and(ending, place > 0))(last)
        return _

    def drain(tau, _):
        for d in range(2):
            passing, copy = pieces(tau, d)[4::2]
            pl.when(passing)(lambda: copy.wait_send())
        return _

    steps_g = max((Z - 1) * K + 1, K - 1 + 2 * (Z - 1)) + 1
    head = min(K, 2)

    def order(k):
        return jnp.where(z < (Z + 1) // 2, Z - 1 - k, k)

    own_part(order(0))
    lax.fori_loop(0, head, step, 0)
    for k in range(1, Z):
        own_part(order(k))
    lax.fori_loop(head, steps_g, step, 0)
    g = gp[z][:Db]

    sq = g * g + FLOOR_VALUE
    rsb[r] = jnp.sum(sq, axis=1, keepdims=True)
    csb[c] = jnp.sum(sq, axis=0, keepdims=True)
    for o in range(1, C):
        c2 = lax.rem(c + o, C)
        send(csb.at[c], csb.at[c], col_ss.at[o], col_rs.at[c], (r, c2))
    for o in range(1, R):
        r2 = lax.rem(r + o, R)
        send(rsb.at[r], rsb.at[r], row_ss.at[o], row_rs.at[r], (r2, c))
    for o in range(1, R):
        r2 = lax.rem(r + o, R)
        arrived(rsb.at[r2], row_rs.at[r2])
    for o in range(1, C):
        c2 = lax.rem(c + o, C)
        arrived(csb.at[c2], col_rs.at[c2])
    row_sum = sum(rsb[k] for k in range(R))
    col_sum = sum(csb[k] for k in range(C))
    new_row = DECAY_RATE * rmc[...] + (1.0 - DECAY_RATE) * row_sum / (R * Fb)
    new_col = DECAY_RATE * cmv[...].reshape(1, Fb) + (1.0 - DECAY_RATE) * col_sum / (C * Db)
    nr_ref[...] = jnp.sum(jnp.where(eye, new_row, 0.0), axis=0)
    nc_ref[...] = new_col[0]
    raw = g / jnp.sqrt(new_row * new_col)
    upd_ref[...] = raw
    local = jnp.sum(jnp.sum(raw * raw, axis=1, keepdims=True), axis=0, keepdims=True)
    loss_local = jnp.sum(loss_a + loss_b, axis=0, keepdims=True)
    lane = lax.broadcasted_iota(jnp.int32, (1, 128), 1)
    stb[me] = jnp.where(lane == 0, local, loss_local)

    def tell(o, wait):
        other = lax.rem(me + o, devices)
        copy = pltpu.make_async_remote_copy(
            src_ref=stb.at[me], dst_ref=stb.at[me], send_sem=st_ss.at[o], recv_sem=st_rs.at[me],
            device_id=(other // C, other % C), device_id_type=MESH,
        )
        if wait:
            copy.wait_send()
            arrived(stb.at[other], st_rs.at[other])
        else:
            copy.start()

    def tell_start(o, _):
        tell(o, False)
        return _

    def tell_wait(o, _):
        tell(o, True)
        return _

    lax.fori_loop(1, devices, tell_start, 0)
    lax.fori_loop(1, devices, tell_wait, 0)
    totals = jnp.sum(stb[...], axis=0)
    rms = jnp.sqrt(totals[:, 0:1] / (C * Db * R * Fb))
    upd_ref[...] = upd_ref[...] / jnp.maximum(1.0, rms / CLIP_LEVEL)
    loss_ref[0] = jnp.sum(jnp.where(lane == 1, totals, 0.0)) / batch
    lax.fori_loop(0, steps_g, drain, 0)
    for wait in finish:
        wait()


def per_device(pooled, hidden, text, weight, row_moment, col_moment, log_scale, bias):
    R, C = lax.axis_size("row"), lax.axis_size("col")
    L, X, Z = LOW, R // CORES, C // LOW
    T, D = pooled.shape
    Db, Fb = weight.shape
    Dp = -(-Db // 16) * 16
    F2 = Z * Dp
    plane = R * L
    texts = X * C * T
    chunk = min(texts, 512)

    K = 3 if Dp % 48 == 0 else 1
    sizes = (R, C, X, Z, T, Db, Dp, Fb, chunk, K)
    vmem = pl.BlockSpec(memory_space=pltpu.VMEM)
    smem = pl.BlockSpec(memory_space=pltpu.SMEM)
    dma = lambda *s: pltpu.SemaphoreType.DMA(s)
    upd, nr, nc, loss = pl.pallas_call(
        functools.partial(kernel, sizes),
        out_shape=(
            jax.ShapeDtypeStruct((Db, Fb), F32),
            jax.ShapeDtypeStruct((Db,), F32),
            jax.ShapeDtypeStruct((Fb,), F32),
            jax.ShapeDtypeStruct((1,), F32),
        ),
        in_specs=[pl.BlockSpec(memory_space=pl.ANY)] * 6 + [smem] * 2,
        out_specs=(vmem,) * 3 + (smem,),
        scratch_shapes=[
            pltpu.VMEM((T, R * Fb), BF16),
            pltpu.VMEM((Db, Fb), F32),
            pltpu.VMEM((T, D), BF16),
            pltpu.VMEM((T, D), BF16),
            pltpu.VMEM((Db,), F32),
            pltpu.VMEM((Fb,), F32),
            pltpu.VMEM((R, T, Fb), BF16),
            pltpu.VMEM((L, T, F2), F32),
            pltpu.VMEM((Db, 1), F32),
            pltpu.VMEM((plane * T, Fb), BF16),
            pltpu.VMEM((F2, Fb), BF16),
            pltpu.VMEM((L, texts, F2), BF16),
            pltpu.VMEM((plane * T, F2), F32),
            pltpu.VMEM((X, L * T, F2), F32),
            pltpu.VMEM((X, L * T, F2), F32),
            pltpu.VMEM((X, L, T, F2), F32),
            pltpu.VMEM((L, T, F2), BF16),
            pltpu.VMEM((L, T, F2), BF16),
            pltpu.VMEM((L, T, F2), F32),
            pltpu.VMEM((L, T, F2), F32),
            pltpu.VMEM((L, T, F2), BF16),
            pltpu.VMEM((plane * T, F2), BF16),
            pltpu.VMEM((F2, plane * T), BF16),
            pltpu.VMEM((Z, Dp, Fb), F32),
            pltpu.VMEM((Z, Dp, Fb), BF16),
            pltpu.VMEM((2, Z, Dp, Fb), BF16),
            pltpu.VMEM((R, Db, 1), F32),
            pltpu.VMEM((C, 1, Fb), F32),
            pltpu.VMEM((R * C, 1, 128), F32),
            dma(6),
            dma(plane), dma(plane), dma(2, Z), dma(Z), dma(2, Z), dma(2, Z, X + L), dma(X * C),
            dma(2, Z, X + L, X + L), dma(X * C, L), dma(X + 1), dma(X), dma(X * L + L), dma(X * L),
            dma(2), dma(2), dma(plane), dma(plane), dma(2, Z, K), dma(2, Z, K),
            dma(R), dma(R), dma(C), dma(C), dma(R * C), dma(R * C),
        ],
        compiler_params=pltpu.CompilerParams(
            has_side_effects=True, collective_id=0, vmem_limit_bytes=60 * 1024 * 1024
        ),
    )(
        hidden, weight, pooled, text, row_moment, col_moment, log_scale[None], bias[None],
    )
    return upd, nr, nc, loss[0]


def solution(mesh):
    return jax.shard_map(
        per_device,
        mesh=mesh,
        in_specs=(
            P(("row", "col"), None),
            P(("row", "col"), None),
            P(("row", "col"), None),
            P("col", "row"),
            P("col"),
            P("row"),
            P(),
            P(),
        ),
        out_specs=(P("col", "row"), P("col"), P("row"), P()),
        check_vma=False,
    )
```

```python
import functools

import jax
import jax.numpy as jnp
from jax import lax
from jax.experimental import pallas as pl
from jax.experimental.pallas import tpu as pltpu
from jax.sharding import PartitionSpec as P

EPSILON = 1e-06
DECAY_RATE = 0.8
CLIP_LEVEL = 1.0
FLOOR_VALUE = 1e-30
CORES = 2
LOW = 2
MESH = pl.DeviceIdType.MESH
F32 = jnp.float32
BF16 = jnp.bfloat16


def dot_nt(a, b):
    return lax.dot_general(a, b, (((1,), (1,)), ((), ())), preferred_element_type=F32)


def kernel(
    sizes,
    hid_in, w_in, pool_in, text_in, rm_in, cm_in, ls_ref, bias_ref,
    upd_ref, nr_ref, nc_ref, loss_ref,
    hv, wv, pv, tv, rmv, cmv, hs, pool, rmc,
    hid, wg, txa, part, pre, summed, proj, img_s, img_r, ug_s, ug_r, mg_s, mga, turned, gp, gz_s, gz,
    rsb, csb, stb, ld,
    hid_ss, hid_rs, w_ss, w_rs, tz_ss, tp_ss, t_rs, td_ss, td_rs, pp_ss, pp_rs, p_ss, p_rs, pair_ss, pair_rs,
    mg_ss, mg_rs, g_ss, g_rs, row_ss, row_rs, col_ss, col_rs, st_ss, st_rs,
):
    R, C, X, Z, T, Db, Dp, Fb, chunk, K, F2, F2p, Fw = sizes
    L = LOW
    plane = R * L
    devices = R * C
    batch = devices * T
    r = lax.axis_index("row")
    c = lax.axis_index("col")
    z, y = c // L, c % L
    x, core = r // CORES, r % CORES
    q = r * L + y
    finish = []
    me = r * C + c
    Dc = Dp // K

    loads = [
        pltpu.make_async_copy(src, dst, ld.at[i])
        for i, (src, dst) in enumerate(
            ((w_in, wv), (hid_in, hv), (text_in, tv), (pool_in, pv), (rm_in, rmv), (cm_in, cmv))
        )
    ]
    for load in loads:
        load.start()
    barrier = pltpu.get_barrier_semaphore()

    def greet(o, _):
        other = lax.rem(me + o, devices)
        pl.semaphore_signal(barrier, inc=1, device_id=(other // C, other % C), device_id_type=MESH)
        return _

    lax.fori_loop(1, devices, greet, 0)

    def send(src, dst, ss, rs, device, cond=None, bulk=False):
        def make():
            return pltpu.make_async_remote_copy(
                src_ref=src, dst_ref=dst, send_sem=ss, recv_sem=rs,
                device_id=device, device_id_type=MESH,
            )

        if cond is None:
            make().start()
        else:
            pl.when(cond)(lambda: make().start())
        if bulk:
            return
        if cond is None:
            finish.append(lambda: make().wait_send())
        else:
            finish.append(lambda: pl.when(cond)(lambda: make().wait_send()))

    def sent(like, ss):
        finish.append(lambda: pltpu.make_async_copy(like, like, ss).wait())

    def arrived(slot, rs):
        pltpu.make_async_copy(slot, slot, rs).wait()

    def plane_peer(o):
        other = lax.rem(q + o, plane)
        return other, other // L, other % L

    def rows(index, count):
        return pl.ds(pl.multiple_of(index * count, count), count)

    def by_half(value, store):
        for h in range(L):
            for k in range(Z):
                at = (k * L + h) * Db
                store(h, k * Dp, value[:, at:at + Db])

    own_slot = x * C + c
    loads[0].wait()
    if Dp != Db:
        wg[rows(z, Dp)] = jnp.zeros((Dp, Fb), BF16)
        txa[:, rows(own_slot, T), :] = jnp.zeros((L, T, Z * Dp), BF16)
        pool[...] = jnp.zeros(pool.shape, F32)
    wg[pl.ds(pl.multiple_of(z * Dp, Dp), Db)] = wv[...].astype(BF16)
    if F2p != F2:
        wg[F2:F2p] = jnp.zeros((F2p - F2, Fb), BF16)
    loads[1].wait()
    for k in range(R):
        hs[k] = hv[:, k * Fb:(k + 1) * Fb]
    hid[rows(q, T)] = hs[r]
    loads[2].wait()
    tf = tv[...].astype(F32)
    tn = tf / jnp.sqrt(jnp.sum(tf * tf, axis=1, keepdims=True) + EPSILON)

    def put_text(h, at, value):
        txa[h, rows(own_slot, T), at:at + Db] = value.astype(BF16)

    by_half(tn, put_text)
    pl.semaphore_wait(barrier, devices - 1)
    for o in range(1, plane):
        _, r2, y2 = plane_peer(o)
        send(hs.at[r2], hid.at[rows(q, T)], hid_ss, hid_rs, (r2, z * L + y2), bulk=True)
    sent(hid.at[pl.ds(0, (plane - 1) * T)], hid_ss)

    def text_place(zs):
        return x * C + zs * L + y

    def neighbours():
        along_x = [(lax.rem(x + o, X), y) for o in range(1, X)]
        return along_x + [(x, lax.rem(y + o, L)) for o in range(1, L)]

    def relay(s):
        for d, direction in enumerate((1, -1)):
            if s == 0 and d:
                continue
            zs = z - direction * s
            has = jnp.logical_and(zs >= 0, zs < Z)
            block = jnp.clip(zs, 0, Z - 1)
            for n, (x2, y2) in enumerate(neighbours()):
                place = x2 * C + block * L + y2
                at = txa.at[:, rows(place, T), :]
                if s:
                    pl.when(has)(lambda: arrived(at, t_rs.at[place]))
                else:
                    arrived(at, t_rs.at[place])
                h = 0 if n < X - 1 else 1
                half = txa.at[h, rows(place, T), :]
                onward = neighbours()[X - 1:] if h == 0 else neighbours()[:X - 1]
                for x3, y3 in onward:
                    send(
                        half, half, td_ss, td_rs,
                        (x3 * CORES + core, z * L + y3), has if s else None, True,
                    )

    def texts_on(s):
        for d, direction in enumerate((1, -1)):
            zs = z - direction * s
            nz = z + direction
            has = jnp.logical_and(zs >= 0, zs < Z)
            go = jnp.logical_and(has, jnp.logical_and(nz >= 0, nz < Z))
            place = text_place(jnp.clip(zs, 0, Z - 1))
            at = txa.at[:, rows(place, T), :]
            if s:
                pl.when(has)(lambda: arrived(at, t_rs.at[place]))
            send(at, at, tz_ss.at[d, s], t_rs.at[place], (r, jnp.clip(nz, 0, Z - 1) * L + y), go)
            if s or d == 0:
                for x2, y2 in neighbours():
                    send(
                        at, at, tp_ss, t_rs.at[place],
                        (x2 * CORES + core, z * L + y2), has if s else None, True,
                    )

    def weights_on(s):
        for d, direction in enumerate((1, -1)):
            zs = z - direction * s
            nz = z + direction
            has = jnp.logical_and(zs >= 0, zs < Z)
            go = jnp.logical_and(has, jnp.logical_and(nz >= 0, nz < Z))
            block = jnp.clip(zs, 0, Z - 1)
            at = wg.at[rows(block, Dp)]
            if s:
                pl.when(has)(lambda: arrived(at, w_rs.at[block]))
            send(at, at, w_ss.at[d, s], w_rs.at[block], (r, jnp.clip(nz, 0, Z - 1) * L + y), go)

    texts_on(0)
    weights_on(0)
    loads[3].wait()

    def put_pool(h, at, value):
        pool[h, :, at:at + Db] = value

    by_half(pv[...].astype(F32), put_pool)
    loads[4].wait()
    loads[5].wait()
    eye = lax.broadcasted_iota(jnp.int32, (Db, Db), 0) == lax.broadcasted_iota(jnp.int32, (Db, Db), 1)
    line = jnp.broadcast_to(rmv[...].reshape(1, Db), (Db, Db))
    rmc[...] = jnp.sum(jnp.where(eye, line, 0.0), axis=1, keepdims=True)
    partner = (x * CORES + (1 - core), c)
    low = z < Z // 2
    spans = (
        (pl.multiple_of(jnp.where(low, 0, Fw), 128), F2p - Fw),
        (pl.multiple_of(jnp.where(low, F2p - Fw, 0), 128), Fw),
    )

    def project(g):
        start, width = spans[g]
        lanes = pl.ds(start, width)
        part[:, lanes] = dot_nt(hid[...], wg[lanes])
        for o in range(1, X + 1):
            x2 = lax.rem(x + o, X)
            send(
                part.at[rows(x2 * CORES + 1 - core, L * T), lanes], pre.at[x2, :, lanes],
                pp_ss, pp_rs.at[x2, g], partner, bulk=True,
            )

    def spread(g):
        start, width = spans[g]
        lanes = pl.ds(start, width)
        for o in range(1, X + 1):
            x2 = lax.rem(x + o, X)
            arrived(pre.at[x2, :, lanes], pp_rs.at[x2, g])
            summed[x2, :, lanes] = part[rows(x2 * CORES + core, L * T), lanes] + pre[x2, :, lanes]
            for k in range(L):
                y2 = lax.rem(y + 1 + k, L)
                if o == X and k == L - 1:
                    proj[x, y, :, lanes] = summed[x, rows(y, T), lanes]
                else:
                    send(
                        summed.at[x2, rows(y2, T), lanes], proj.at[x, y, :, lanes], p_ss,
                        p_rs.at[g], (x2 * CORES + core, z * L + y2), bulk=True,
                    )

    def gathered(g):
        start, width = spans[g]
        arrived(part.at[pl.ds(0, (X * L - 1) * T), pl.ds(start, width)], p_rs.at[g])

    for s in range(1, Z):
        texts_on(s)
        if s == Z - 1:
            spread(0)
        else:
            weights_on(s)
        relay(s - 1)
        if s == Z - 2:
            arrived(hid.at[pl.ds(0, (plane - 1) * T)], hid_rs)
            project(0)
    weights_on(Z - 1)
    project(1)
    count = (X - 1) * (L - 1) * Z * T
    sent(txa.at[:, pl.ds(0, count), :], td_ss)
    sent(txa.at[:, pl.ds(0, Z * (X + L - 2) * T), :], tp_ss)
    sent(part.at[pl.ds(0, X * L * T)], pp_ss)
    sent(part.at[pl.ds(0, (X * L - 1) * T)], p_ss)
    relay(Z - 1)
    spread(1)
    gathered(0)
    gathered(1)
    mixed = []
    for h in range(L):
        total = proj[0, h]
        for k in range(1, X):
            total = total + proj[k, h]
        mixed.append(pool[h] + total[:, :F2])
    square = sum(jnp.sum(m * m, axis=1, keepdims=True) for m in mixed)
    length = jnp.sqrt(square + EPSILON)
    unit = [m / length for m in mixed]
    for h in range(L):
        img_s[h] = unit[h].astype(BF16)
    send(img_s, img_r, pair_ss.at[0], pair_rs.at[0], partner)

    arrived(txa.at[:, pl.ds(0, count), :], td_rs)

    scale = jnp.exp(jnp.full((1, 1), ls_ref[0], F32))
    bias = jnp.full((1, 1), bias_ref[0], F32)
    steps = X * C * T // chunk

    def pairs(images, own):
        halves = [images[h] for h in range(L)]

        def step(i, carry):
            loss, grads = carry
            cut = pl.ds(pl.multiple_of(i * chunk, chunk), chunk)
            texts = [txa[h, cut, :] for h in range(L)]
            logits = scale * sum(dot_nt(halves[h], texts[h]) for h in range(L)) + bias
            if own:
                row_id = lax.broadcasted_iota(jnp.int32, logits.shape, 0) + own_slot * T
                col_id = lax.broadcasted_iota(jnp.int32, logits.shape, 1) + i * chunk
                sign = jnp.where(row_id == col_id, F32(1.0), F32(-1.0))
            else:
                sign = F32(-1.0)
            u = -sign * logits
            e = jnp.exp(-jnp.abs(u))
            loss = loss + jnp.sum(jnp.maximum(u, 0.0) + jnp.log1p(e), axis=1, keepdims=True)
            sig = jnp.where(u >= 0, F32(1.0), e) / (1.0 + e)
            pg = (-sign * sig / batch).astype(BF16)
            grads = tuple(
                grads[h] + jnp.dot(pg, texts[h], preferred_element_type=F32) for h in range(L)
            )
            return loss, grads

        zero = (jnp.zeros((T, 1), F32), tuple(jnp.zeros((T, Z * Dp), F32) for _ in range(L)))
        if steps == 1:
            return step(0, zero)
        return lax.fori_loop(0, steps, step, zero)

    arrived(img_r, pair_rs.at[0])
    loss_b, grads_b = pairs(img_r, False)
    for h in range(L):
        ug_s[h] = scale * grads_b[h]
    send(ug_s, ug_r, pair_ss.at[1], pair_rs.at[1], partner)
    loss_a, grads_a = pairs(img_s, True)
    arrived(ug_r, pair_rs.at[1])
    ug = [scale * grads_a[h] + ug_r[h] for h in range(L)]
    inner = sum(jnp.sum(unit[h] * ug[h], axis=1, keepdims=True) for h in range(L))
    for h in range(L):
        mg_s[h] = ((ug[h] - unit[h] * inner) / length).astype(BF16)
    others = [
        (lax.rem(x + ox, X), lax.rem(y + oy, L))
        for ox in reversed(range(X)) for oy in reversed(range(L)) if ox or oy
    ]
    for x2, y2 in others:
        send(
            mg_s.at[y2], mga.at[rows(q, T)], mg_ss, mg_rs.at[q],
            (x2 * CORES + core, z * L + y2), bulk=True,
        )
    send(mg_s.at[y], mga.at[rows(q, T)], mg_ss, mg_rs.at[q], partner, bulk=True)
    mga[rows(q, T)] = mg_s[y]
    for x2, y2 in others:
        source = (x2 * CORES + core) * L + y2
        at = mga.at[rows(source, T)]
        arrived(at, mg_rs.at[source])
        send(at, at, mg_ss, mg_rs.at[source], partner, bulk=True)
    sent(mga.at[pl.ds(0, (plane - 1) * T)], mg_ss)
    for x2, y2 in [(x, y)] + others:
        source = (x2 * CORES + 1 - core) * L + y2
        arrived(mga.at[rows(source, T)], mg_rs.at[source])

    turned[...] = mga[...].T

    def own_part(zd):
        gp[zd] = jnp.dot(turned[rows(zd, Dp)], hid[...], preferred_element_type=F32)

    def pieces(tau, d):
        place = z if d == 0 else Z - 1 - z
        i = tau - 2 * place
        zd = jnp.clip(i, 0, Z * K - 1) // K
        k = jnp.clip(i, 0, Z * K - 1) % K
        zd = Z - 1 - zd if d == 0 else zd
        beyond = zd > z if d == 0 else zd < z
        ready = jnp.logical_and(i >= 0, i < Z * K)
        cut = rows(k, Dc)
        copy = pltpu.make_async_remote_copy(
            src_ref=gz_s.at[zd, cut], dst_ref=gz.at[d, zd, cut],
            send_sem=g_ss, recv_sem=g_rs.at[d, zd, k],
            device_id=(r, jnp.clip(z + (1 if d == 0 else -1), 0, Z - 1) * L + y), device_id_type=MESH,
        )
        return place, zd, k, cut, jnp.logical_and(ready, beyond), jnp.logical_and(ready, zd == z), copy

    def step(tau, _):
        for d in range(2):
            place, zd, k, cut, passing, ending, copy = pieces(tau, d)
            at = gz.at[d, zd, cut]

            def first():
                gz_s[zd, cut] = gp[zd, cut].astype(BF16)
                copy.start()

            def onward():
                arrived(at, g_rs.at[d, zd, k])
                gz_s[zd, cut] = (gp[zd, cut] + at[...].astype(F32)).astype(BF16)
                copy.start()

            def last():
                arrived(at, g_rs.at[d, zd, k])
                gp[zd, cut] = gp[zd, cut] + at[...].astype(F32)

            pl.when(jnp.logical_and(passing, place == 0))(first)
            pl.when(jnp.logical_and(passing, place > 0))(onward)
            pl.when(jnp.logical_and(ending, place > 0))(last)
        return _

    steps_g = max((Z - 1) * K + 1, K - 1 + 2 * (Z - 1)) + 1
    head = min(K, 2)

    def order(k):
        return jnp.where(z < (Z + 1) // 2, Z - 1 - k, k)

    own_part(order(0))
    lax.fori_loop(0, head, step, 0)
    for k in range(1, Z):
        own_part(order(k))
    sent(gz_s.at[pl.ds(0, Z - 1)], g_ss)
    lax.fori_loop(head, steps_g, step, 0)
    g = gp[z][:Db]

    sq = g * g + FLOOR_VALUE
    rsb[r] = jnp.sum(sq, axis=1, keepdims=True)
    csb[c] = jnp.sum(sq, axis=0, keepdims=True)
    for o in range(1, C):
        c2 = lax.rem(c + o, C)
        send(csb.at[c], csb.at[c], col_ss, col_rs, (r, c2), bulk=True)
    for o in range(1, R):
        r2 = lax.rem(r + o, R)
        send(rsb.at[r], rsb.at[r], row_ss, row_rs, (r2, c), bulk=True)
    sent(csb.at[pl.ds(0, C - 1)], col_ss)
    sent(rsb.at[pl.ds(0, R - 1)], row_ss)
    arrived(rsb.at[pl.ds(0, R - 1)], row_rs)
    arrived(csb.at[pl.ds(0, C - 1)], col_rs)
    row_sum = sum(rsb[k] for k in range(R))
    col_sum = sum(csb[k] for k in range(C))
    new_row = DECAY_RATE * rmc[...] + (1.0 - DECAY_RATE) * row_sum / (R * Fb)
    new_col = DECAY_RATE * cmv[...].reshape(1, Fb) + (1.0 - DECAY_RATE) * col_sum / (C * Db)
    nr_ref[...] = jnp.sum(jnp.where(eye, new_row, 0.0), axis=0)
    nc_ref[...] = new_col[0]
    raw = g / jnp.sqrt(new_row * new_col)
    upd_ref[...] = raw
    local = jnp.sum(jnp.sum(raw * raw, axis=1, keepdims=True), axis=0, keepdims=True)
    loss_local = jnp.sum(loss_a + loss_b, axis=0, keepdims=True)
    lane = lax.broadcasted_iota(jnp.int32, (1, 128), 1)
    stb[me] = jnp.where(lane == 0, local, loss_local)

    def tell(o, _):
        other = lax.rem(me + o, devices)
        pltpu.make_async_remote_copy(
            src_ref=stb.at[me], dst_ref=stb.at[me], send_sem=st_ss, recv_sem=st_rs,
            device_id=(other // C, other % C), device_id_type=MESH,
        ).start()
        return _

    lax.fori_loop(1, devices, tell, 0)
    sent(stb.at[pl.ds(0, devices - 1)], st_ss)
    arrived(stb.at[pl.ds(0, devices - 1)], st_rs)
    totals = jnp.sum(stb[...], axis=0)
    rms = jnp.sqrt(totals[:, 0:1] / (C * Db * R * Fb))
    upd_ref[...] = upd_ref[...] / jnp.maximum(1.0, rms / CLIP_LEVEL)
    loss_ref[0] = jnp.sum(jnp.where(lane == 1, totals, 0.0)) / batch
    for wait in finish:
        wait()


def per_device(pooled, hidden, text, weight, row_moment, col_moment, log_scale, bias):
    R, C = lax.axis_size("row"), lax.axis_size("col")
    L, X, Z = LOW, R // CORES, C // LOW
    T, D = pooled.shape
    Db, Fb = weight.shape
    Dp = -(-Db // 16) * 16
    F2 = Z * Dp
    plane = R * L
    texts = X * C * T
    chunk = min(texts, 512)

    K = 3 if Dp % 48 == 0 else 1
    F2p = -(-F2 // 128) * 128
    Fw = max(-(-Dp // 128) * 128, F2p - (F2 - Dp) // 128 * 128)
    sizes = (R, C, X, Z, T, Db, Dp, Fb, chunk, K, F2, F2p, Fw)
    vmem = pl.BlockSpec(memory_space=pltpu.VMEM)
    smem = pl.BlockSpec(memory_space=pltpu.SMEM)
    dma = lambda *s: pltpu.SemaphoreType.DMA(s)
    one = pltpu.SemaphoreType.DMA
    upd, nr, nc, loss = pl.pallas_call(
        functools.partial(kernel, sizes),
        out_shape=(
            jax.ShapeDtypeStruct((Db, Fb), F32),
            jax.ShapeDtypeStruct((Db,), F32),
            jax.ShapeDtypeStruct((Fb,), F32),
            jax.ShapeDtypeStruct((1,), F32),
        ),
        in_specs=[pl.BlockSpec(memory_space=pl.ANY)] * 6 + [smem] * 2,
        out_specs=(vmem,) * 3 + (smem,),
        scratch_shapes=[
            pltpu.VMEM((T, R * Fb), BF16),
            pltpu.VMEM((Db, Fb), F32),
            pltpu.VMEM((T, D), BF16),
            pltpu.VMEM((T, D), BF16),
            pltpu.VMEM((Db,), F32),
            pltpu.VMEM((Fb,), F32),
            pltpu.VMEM((R, T, Fb), BF16),
            pltpu.VMEM((L, T, F2), F32),
            pltpu.VMEM((Db, 1), F32),
            pltpu.VMEM((plane * T, Fb), BF16),
            pltpu.VMEM((F2p, Fb), BF16),
            pltpu.VMEM((L, texts, F2), BF16),
            pltpu.VMEM((plane * T, F2p), F32),
            pltpu.VMEM((X, L * T, F2p), F32),
            pltpu.VMEM((X, L * T, F2p), F32),
            pltpu.VMEM((X, L, T, F2p), F32),
            pltpu.VMEM((L, T, F2), BF16),
            pltpu.VMEM((L, T, F2), BF16),
            pltpu.VMEM((L, T, F2), F32),
            pltpu.VMEM((L, T, F2), F32),
            pltpu.VMEM((L, T, F2), BF16),
            pltpu.VMEM((plane * T, F2), BF16),
            pltpu.VMEM((F2, plane * T), BF16),
            pltpu.VMEM((Z, Dp, Fb), F32),
            pltpu.VMEM((Z, Dp, Fb), BF16),
            pltpu.VMEM((2, Z, Dp, Fb), BF16),
            pltpu.VMEM((R, Db, 1), F32),
            pltpu.VMEM((C, 1, Fb), F32),
            pltpu.VMEM((R * C, 1, 128), F32),
            dma(6),
            one, one, dma(2, Z), dma(Z), dma(2, Z), one, dma(X * C), one, one,
            one, dma(X, 2), one, dma(2), dma(2), dma(2),
            one, dma(plane), one, dma(2, Z, K), one, one, one, one, one, one,
        ],
        compiler_params=pltpu.CompilerParams(
            has_side_effects=True, collective_id=0, vmem_limit_bytes=60 * 1024 * 1024
        ),
    )(
        hidden, weight, pooled, text, row_moment, col_moment, log_scale[None], bias[None],
    )
    return upd, nr, nc, loss[0]


def solution(mesh):
    return jax.shard_map(
        per_device,
        mesh=mesh,
        in_specs=(
            P(("row", "col"), None),
            P(("row", "col"), None),
            P(("row", "col"), None),
            P("col", "row"),
            P("col"),
            P("row"),
            P(),
            P(),
        ),
        out_specs=(P("col", "row"), P("col"), P("row"), P()),
        check_vma=False,
    )
```

```python
import functools

import jax
import jax.numpy as jnp
from jax import lax
from jax.experimental import pallas as pl
from jax.experimental.pallas import tpu as pltpu
from jax.sharding import PartitionSpec as P

EPSILON = 1e-06
DECAY_RATE = 0.8
CLIP_LEVEL = 1.0
FLOOR_VALUE = 1e-30
CORES = 2
LOW = 2
MESH = pl.DeviceIdType.MESH
F32 = jnp.float32
BF16 = jnp.bfloat16


def dot_nt(a, b):
    return lax.dot_general(a, b, (((1,), (1,)), ((), ())), preferred_element_type=F32)


def kernel(
    sizes,
    hid_in, w_in, pool_in, text_in, rm_in, cm_in, ls_ref, bias_ref,
    upd_ref, nr_ref, nc_ref, loss_ref,
    hv, wv, pv, tv, rmv, cmv, hs, pool, rmc,
    hid, wg, txa, part, pre, summed, proj, mix, imgs, ug_s, ug_r, mg_s, mga, turned, gp, gz_s, gz,
    rsb, csb, stb, ld,
    hid_ss, hid_rs, hx_rs, w_ss, w_rs, tz_ss, tp_ss, t_rs, td_ss, td_rs, pp_ss, pp_rs, p_ss, p_rs, pair_ss, pair_rs,
    mg_ss, mg_rs, g_ss, g_rs, row_ss, row_rs, col_ss, col_rs, st_ss, st_rs,
):
    R, C, X, Z, T, Db, Dp, Fb, K, F2, F2p, Fw = sizes
    L = LOW
    plane = R * L
    devices = R * C
    batch = devices * T
    r = lax.axis_index("row")
    c = lax.axis_index("col")
    z, y = c // L, c % L
    x, core = r // CORES, r % CORES
    q = r * L + y
    finish = []
    me = r * C + c
    Dc = Dp // K

    loads = [
        pltpu.make_async_copy(src, dst, ld.at[i])
        for i, (src, dst) in enumerate(
            ((w_in, wv), (hid_in, hv), (text_in, tv), (pool_in, pv), (rm_in, rmv), (cm_in, cmv))
        )
    ]
    for load in loads:
        load.start()
    barrier = pltpu.get_barrier_semaphore()

    def greet(device):
        pl.semaphore_signal(barrier, inc=1, device_id=device, device_id_type=MESH)

    for o in range(1, plane):
        other = lax.rem(q + o, plane)
        greet((other // L, z * L + other % L))
    pl.when(z > 0)(lambda: greet((r, c - L)))
    pl.when(z < Z - 1)(lambda: greet((r, c + L)))

    def send(src, dst, ss, rs, device, cond=None, bulk=False):
        def make():
            return pltpu.make_async_remote_copy(
                src_ref=src, dst_ref=dst, send_sem=ss, recv_sem=rs,
                device_id=device, device_id_type=MESH,
            )

        if cond is None:
            make().start()
        else:
            pl.when(cond)(lambda: make().start())
        if bulk:
            return
        if cond is None:
            finish.append(lambda: make().wait_send())
        else:
            finish.append(lambda: pl.when(cond)(lambda: make().wait_send()))

    def sent(like, ss):
        finish.append(lambda: pltpu.make_async_copy(like, like, ss).wait())

    def arrived(slot, rs):
        pltpu.make_async_copy(slot, slot, rs).wait()

    def rows(index, count):
        return pl.ds(pl.multiple_of(index * count, count), count)

    def by_half(value, store):
        for h in range(L):
            for k in range(Z):
                at = (k * L + h) * Db
                store(h * F2 + k * Dp, value[:, at:at + Db])

    own_slot = (z * X + x) * L + y
    loads[0].wait()
    if Dp != Db:
        wg[rows(z, Dp)] = jnp.zeros((Dp, Fb), BF16)
        txa[rows(own_slot, T)] = jnp.zeros((T, L * F2), BF16)
        pool[...] = jnp.zeros(pool.shape, F32)
    wg[pl.ds(pl.multiple_of(z * Dp, Dp), Db)] = wv[...].astype(BF16)
    if F2p != F2:
        wg[F2:F2p] = jnp.zeros((F2p - F2, Fb), BF16)
    loads[1].wait()
    for k in range(R):
        hs[k] = hv[:, k * Fb:(k + 1) * Fb]
    hid[rows(q, T)] = hs[r]
    loads[2].wait()
    tf = tv[...].astype(F32)
    tn = tf / jnp.sqrt(jnp.sum(tf * tf, axis=1, keepdims=True) + EPSILON)

    def put_text(at, value):
        txa[rows(own_slot, T), at:at + Db] = value.astype(BF16)

    by_half(tn, put_text)
    pl.semaphore_wait(barrier, plane - 1 + jnp.where(z > 0, 1, 0) + jnp.where(z < Z - 1, 1, 0))
    across = [lax.rem(x + o, X) for o in range(1, X)]
    beside = [lax.rem(y + o, L) for o in range(1, L)]
    partner = (x * CORES + (1 - core), c)
    own_rows = hid.at[rows(q, T)]
    for x2 in across:
        for k in range(CORES):
            r2 = x2 * CORES + k
            send(hs.at[r2], own_rows, hid_ss, hx_rs, (r2, c), bulk=True)
    for y2 in beside:
        for k in range(CORES):
            r2 = x * CORES + k
            send(hs.at[r2], own_rows, hid_ss, hid_rs, (r2, z * L + y2), bulk=True)
    send(hs.at[partner[0]], own_rows, hid_ss, hid_rs, partner, bulk=True)
    crossing = (X - 1) * CORES
    relayed = crossing * (L - 1)
    direct = crossing + CORES * (L - 1) + 1

    def hidden_on():
        arrived(hid.at[pl.ds(0, crossing * T)], hx_rs)
        for x2 in across:
            for k in range(CORES):
                at = hid.at[rows((x2 * CORES + k) * L + y, T)]
                for y2 in beside:
                    send(at, at, hid_ss, hid_rs, (r, z * L + y2), bulk=True)
        sent(hid.at[pl.ds(0, (direct + relayed) * T)], hid_ss)

    def text_place(zs):
        return (zs * X + x) * L + y

    def neighbours():
        along_x = [(lax.rem(x + o, X), y) for o in range(1, X)]
        return along_x + [(x, lax.rem(y + o, L)) for o in range(1, L)]

    split = T // 4
    low = z < Z // 2
    final = jnp.where(low, Z - 1, 0)

    def relay(s):
        for d, direction in enumerate((1, -1)):
            if s == 0 and d:
                continue
            zs = z - direction * s
            has = jnp.logical_and(zs >= 0, zs < Z)
            block = jnp.clip(zs, 0, Z - 1)
            for n, (x2, y2) in enumerate(neighbours()):
                place = (block * X + x2) * L + y2
                at = txa.at[rows(place, T)]
                if s:
                    pl.when(has)(lambda: arrived(at, t_rs.at[place]))
                else:
                    arrived(at, t_rs.at[place])
                h = 0 if n < X - 1 else 1
                part_at = pl.multiple_of(place * T + h * split, split)
                half = txa.at[pl.ds(part_at, T - split if h else split)]
                onward = neighbours()[X - 1:] if h == 0 else neighbours()[:X - 1]
                for x3, y3 in onward:
                    send(
                        half, half, td_ss, td_rs.at[jnp.where(block == final, 1, 0)],
                        (x3 * CORES + core, z * L + y3), has if s else None, True,
                    )

    def texts_on(s):
        for d, direction in enumerate((1, -1)):
            zs = z - direction * s
            nz = z + direction
            has = jnp.logical_and(zs >= 0, zs < Z)
            go = jnp.logical_and(has, jnp.logical_and(nz >= 0, nz < Z))
            place = text_place(jnp.clip(zs, 0, Z - 1))
            at = txa.at[rows(place, T)]
            if s:
                pl.when(has)(lambda: arrived(at, t_rs.at[place]))
            send(at, at, tz_ss.at[d, s], t_rs.at[place], (r, jnp.clip(nz, 0, Z - 1) * L + y), go)
            if s or d == 0:
                for x2, y2 in neighbours():
                    send(
                        at, at, tp_ss, t_rs.at[place],
                        (x2 * CORES + core, z * L + y2), has if s else None, True,
                    )

    def weights_on(s):
        for d, direction in enumerate((1, -1)):
            zs = z - direction * s
            nz = z + direction
            has = jnp.logical_and(zs >= 0, zs < Z)
            go = jnp.logical_and(has, jnp.logical_and(nz >= 0, nz < Z))
            block = jnp.clip(zs, 0, Z - 1)
            at = wg.at[rows(block, Dp)]
            if s:
                pl.when(has)(lambda: arrived(at, w_rs.at[block]))
            send(at, at, w_ss.at[d, s], w_rs.at[block], (r, jnp.clip(nz, 0, Z - 1) * L + y), go)

    texts_on(0)
    weights_on(0)
    loads[3].wait()

    def put_pool(at, value):
        pool[:, at:at + Db] = value

    by_half(pv[...].astype(F32), put_pool)
    loads[4].wait()
    loads[5].wait()
    eye = lax.broadcasted_iota(jnp.int32, (Db, Db), 0) == lax.broadcasted_iota(jnp.int32, (Db, Db), 1)
    line = jnp.broadcast_to(rmv[...].reshape(1, Db), (Db, Db))
    rmc[...] = jnp.sum(jnp.where(eye, line, 0.0), axis=1, keepdims=True)
    spans = (
        (pl.multiple_of(jnp.where(low, 0, Fw), 128), F2p - Fw),
        (pl.multiple_of(jnp.where(low, F2p - Fw, 0), 128), Fw),
    )

    def project(g):
        start, width = spans[g]
        lanes = pl.ds(start, width)
        part[:, lanes] = dot_nt(hid[...], wg[lanes])
        for o in range(1, X + 1):
            x2 = lax.rem(x + o, X)
            send(
                part.at[rows(x2 * CORES + 1 - core, L * T), lanes], pre.at[x2, :, lanes],
                pp_ss, pp_rs.at[x2, g], partner, bulk=True,
            )

    def spread(g):
        start, width = spans[g]
        lanes = pl.ds(start, width)
        for o in range(1, X + 1):
            x2 = lax.rem(x + o, X)
            arrived(pre.at[x2, :, lanes], pp_rs.at[x2, g])
            summed[x2, :, lanes] = part[rows(x2 * CORES + core, L * T), lanes] + pre[x2, :, lanes]
            for k in range(L):
                y2 = lax.rem(y + 1 + k, L)
                if o == X and k == L - 1:
                    proj[x, y, :, lanes] = summed[x, rows(y, T), lanes]
                else:
                    send(
                        summed.at[x2, rows(y2, T), lanes], proj.at[x, y, :, lanes], p_ss,
                        p_rs.at[g], (x2 * CORES + core, z * L + y2), bulk=True,
                    )

    def gathered(g):
        start, width = spans[g]
        arrived(part.at[pl.ds(0, (X * L - 1) * T), pl.ds(start, width)], p_rs.at[g])

    for s in range(1, Z):
        texts_on(s)
        if s == 1:
            hidden_on()
        if s == Z - 1:
            spread(0)
        else:
            weights_on(s)
        relay(s - 1)
        if s == Z - 2:
            arrived(hid.at[pl.ds(0, (plane - 1 - crossing) * T)], hid_rs)
            project(0)
    weights_on(Z - 1)
    project(1)
    sent(part.at[pl.ds(0, X * L * T)], pp_ss)
    sent(part.at[pl.ds(0, (X * L - 1) * T)], p_ss)
    relay(Z - 1)
    spread(1)
    pairs_each = (X - 1) * (L - 1) * T
    sent(txa.at[pl.ds(0, Z * pairs_each)], td_ss)
    sent(txa.at[pl.ds(0, Z * (X + L - 2) * T)], tp_ss)
    gathered(0)
    gathered(1)
    for h in range(L):
        total = proj[0, h]
        for k in range(1, X):
            total = total + proj[k, h]
        mix[:, h * F2:(h + 1) * F2] = total[:, :F2]
    mixed = mix[...] + pool[...]
    length = jnp.sqrt(jnp.sum(mixed * mixed, axis=1, keepdims=True) + EPSILON)
    unit = mixed / length
    imgs[:T] = unit.astype(BF16)
    theirs = imgs.at[pl.ds(T, T)]
    send(imgs.at[pl.ds(0, T)], theirs, pair_ss.at[0], pair_rs.at[0], partner)
    scale = jnp.exp(jnp.full((1, 1), ls_ref[0], F32))
    bias = jnp.full((1, 1), bias_ref[0], F32)
    width = X * L * T

    def pairs(top, count, zs):
        images = imgs[top:top + count]
        texts = txa[rows(zs, width)]
        logits = scale * dot_nt(images, texts) + bias
        row_id = lax.broadcasted_iota(jnp.int32, logits.shape, 0) + top
        col_id = lax.broadcasted_iota(jnp.int32, logits.shape, 1) + (zs * width - own_slot * T)
        match = jnp.logical_and(row_id == col_id, row_id < T)
        u = jnp.where(match, -logits, logits)
        e = jnp.exp(-jnp.abs(u))
        loss = jnp.sum(jnp.maximum(u, 0.0) + jnp.log1p(e), axis=1, keepdims=True)
        sig = jnp.where(u >= 0, F32(1.0), e) / (1.0 + e)
        pg = (jnp.where(match, -sig, sig) / batch).astype(BF16)
        return loss, jnp.dot(pg, texts, preferred_element_type=F32)

    def more(k, carry):
        loss, grads = pairs(0, 2 * T, jnp.where(low, k, Z - 1 - k))
        return carry[0] + loss, carry[1] + grads

    arrived(txa.at[pl.ds(0, (Z - 1) * pairs_each)], td_rs.at[0])
    arrived(theirs, pair_rs.at[0])
    carry = (jnp.zeros((2 * T, 1), F32), jnp.zeros((2 * T, L * F2), F32))
    if Z <= 4:
        for k in range(Z - 1):
            carry = more(k, carry)
    else:
        carry = lax.fori_loop(0, Z - 1, more, carry)
    loss_most, grads = carry
    arrived(txa.at[pl.ds(0, pairs_each)], td_rs.at[1])
    loss_b, grads_b = pairs(T, T, final)
    ug_s[...] = scale * (grads[T:] + grads_b)
    send(ug_s, ug_r, pair_ss.at[1], pair_rs.at[1], partner)
    loss_a, grads_a = pairs(0, T, final)
    arrived(ug_r, pair_rs.at[1])
    ug = scale * (grads[:T] + grads_a) + ug_r[...]
    inner = jnp.sum(unit * ug, axis=1, keepdims=True)
    mg = ((ug - unit * inner) / length).astype(BF16)
    for h in range(L):
        mg_s[h] = mg[:, h * F2:(h + 1) * F2]
    others = [
        (lax.rem(x + ox, X), lax.rem(y + oy, L))
        for ox in reversed(range(X)) for oy in reversed(range(L)) if ox or oy
    ]
    for x2, y2 in others:
        send(
            mg_s.at[y2], mga.at[rows(q, T)], mg_ss, mg_rs.at[q],
            (x2 * CORES + core, z * L + y2), bulk=True,
        )
    send(mg_s.at[y], mga.at[rows(q, T)], mg_ss, mg_rs.at[q], partner, bulk=True)
    mga[rows(q, T)] = mg_s[y]
    for x2, y2 in others:
        source = (x2 * CORES + core) * L + y2
        at = mga.at[rows(source, T)]
        arrived(at, mg_rs.at[source])
        send(at, at, mg_ss, mg_rs.at[source], partner, bulk=True)
    sent(mga.at[pl.ds(0, (plane - 1) * T)], mg_ss)
    for x2, y2 in [(x, y)] + others:
        source = (x2 * CORES + 1 - core) * L + y2
        arrived(mga.at[rows(source, T)], mg_rs.at[source])

    turned[...] = mga[...].T

    def own_part(zd):
        gp[zd] = jnp.dot(turned[rows(zd, Dp)], hid[...], preferred_element_type=F32)

    def pieces(tau, d):
        place = z if d == 0 else Z - 1 - z
        i = tau - 2 * place
        zd = jnp.clip(i, 0, Z * K - 1) // K
        k = jnp.clip(i, 0, Z * K - 1) % K
        zd = Z - 1 - zd if d == 0 else zd
        beyond = zd > z if d == 0 else zd < z
        ready = jnp.logical_and(i >= 0, i < Z * K)
        cut = rows(k, Dc)
        copy = pltpu.make_async_remote_copy(
            src_ref=gz_s.at[zd, cut], dst_ref=gz.at[d, zd, cut],
            send_sem=g_ss, recv_sem=g_rs.at[d, zd, k],
            device_id=(r, jnp.clip(z + (1 if d == 0 else -1), 0, Z - 1) * L + y), device_id_type=MESH,
        )
        return place, zd, k, cut, jnp.logical_and(ready, beyond), jnp.logical_and(ready, zd == z), copy

    def step(tau, _):
        for d in range(2):
            place, zd, k, cut, passing, ending, copy = pieces(tau, d)
            at = gz.at[d, zd, cut]

            def first():
                gz_s[zd, cut] = gp[zd, cut].astype(BF16)
                copy.start()

            def onward():
                arrived(at, g_rs.at[d, zd, k])
                gz_s[zd, cut] = (gp[zd, cut] + at[...].astype(F32)).astype(BF16)
                copy.start()

            def last():
                arrived(at, g_rs.at[d, zd, k])
                gp[zd, cut] = gp[zd, cut] + at[...].astype(F32)

            pl.when(jnp.logical_and(passing, place == 0))(first)
            pl.when(jnp.logical_and(passing, place > 0))(onward)
            pl.when(jnp.logical_and(ending, place > 0))(last)
        return _

    steps_g = max((Z - 1) * K + 1, K - 1 + 2 * (Z - 1)) + 1
    head = min(K, 2)

    def order(k):
        return jnp.where(z < (Z + 1) // 2, Z - 1 - k, k)

    own_part(order(0))
    lax.fori_loop(0, head, step, 0)
    for k in range(1, Z):
        own_part(order(k))
    sent(gz_s.at[pl.ds(0, Z - 1)], g_ss)
    lax.fori_loop(head, steps_g, step, 0)
    g = gp[z][:Db]

    sq = g * g + FLOOR_VALUE
    rsb[r] = jnp.sum(sq, axis=1, keepdims=True)
    csb[c] = jnp.sum(sq, axis=0, keepdims=True)
    for o in range(1, C):
        c2 = lax.rem(c + o, C)
        send(csb.at[c], csb.at[c], col_ss, col_rs, (r, c2), bulk=True)
    for o in range(1, R):
        r2 = lax.rem(r + o, R)
        send(rsb.at[r], rsb.at[r], row_ss, row_rs, (r2, c), bulk=True)
    sent(csb.at[pl.ds(0, C - 1)], col_ss)
    sent(rsb.at[pl.ds(0, R - 1)], row_ss)
    arrived(rsb.at[pl.ds(0, R - 1)], row_rs)
    arrived(csb.at[pl.ds(0, C - 1)], col_rs)
    row_sum = sum(rsb[k] for k in range(R))
    col_sum = sum(csb[k] for k in range(C))
    new_row = DECAY_RATE * rmc[...] + (1.0 - DECAY_RATE) * row_sum / (R * Fb)
    new_col = DECAY_RATE * cmv[...].reshape(1, Fb) + (1.0 - DECAY_RATE) * col_sum / (C * Db)
    nr_ref[...] = jnp.sum(jnp.where(eye, new_row, 0.0), axis=0)
    nc_ref[...] = new_col[0]
    raw = g / jnp.sqrt(new_row * new_col)
    upd_ref[...] = raw
    local = jnp.sum(jnp.sum(raw * raw, axis=1, keepdims=True), axis=0, keepdims=True)
    loss_local = jnp.sum(loss_a + loss_b, axis=0, keepdims=True) + jnp.sum(loss_most, axis=0, keepdims=True)
    lane = lax.broadcasted_iota(jnp.int32, (1, 128), 1)
    stb[me] = jnp.where(lane == 0, local, loss_local)

    def tell(o, _):
        other = lax.rem(me + o, devices)
        pltpu.make_async_remote_copy(
            src_ref=stb.at[me], dst_ref=stb.at[me], send_sem=st_ss, recv_sem=st_rs,
            device_id=(other // C, other % C), device_id_type=MESH,
        ).start()
        return _

    lax.fori_loop(1, devices, tell, 0)
    sent(stb.at[pl.ds(0, devices - 1)], st_ss)
    arrived(stb.at[pl.ds(0, devices - 1)], st_rs)
    totals = jnp.sum(stb[...], axis=0)
    rms = jnp.sqrt(totals[:, 0:1] / (C * Db * R * Fb))
    upd_ref[...] = upd_ref[...] / jnp.maximum(1.0, rms / CLIP_LEVEL)
    loss_ref[0] = jnp.sum(jnp.where(lane == 1, totals, 0.0)) / batch
    for wait in finish:
        wait()


def per_device(pooled, hidden, text, weight, row_moment, col_moment, log_scale, bias):
    R, C = lax.axis_size("row"), lax.axis_size("col")
    L, X, Z = LOW, R // CORES, C // LOW
    T, D = pooled.shape
    Db, Fb = weight.shape
    Dp = -(-Db // 16) * 16
    F2 = Z * Dp
    plane = R * L
    texts = X * C * T

    K = 3 if Dp % 48 == 0 else 1
    F2p = -(-F2 // 128) * 128
    Fw = max(-(-Dp // 128) * 128, F2p - (F2 - Dp) // 128 * 128)
    sizes = (R, C, X, Z, T, Db, Dp, Fb, K, F2, F2p, Fw)
    vmem = pl.BlockSpec(memory_space=pltpu.VMEM)
    smem = pl.BlockSpec(memory_space=pltpu.SMEM)
    dma = lambda *s: pltpu.SemaphoreType.DMA(s)
    one = pltpu.SemaphoreType.DMA
    upd, nr, nc, loss = pl.pallas_call(
        functools.partial(kernel, sizes),
        out_shape=(
            jax.ShapeDtypeStruct((Db, Fb), F32),
            jax.ShapeDtypeStruct((Db,), F32),
            jax.ShapeDtypeStruct((Fb,), F32),
            jax.ShapeDtypeStruct((1,), F32),
        ),
        in_specs=[pl.BlockSpec(memory_space=pl.ANY)] * 6 + [smem] * 2,
        out_specs=(vmem,) * 3 + (smem,),
        scratch_shapes=[
            pltpu.VMEM((T, R * Fb), BF16),
            pltpu.VMEM((Db, Fb), F32),
            pltpu.VMEM((T, D), BF16),
            pltpu.VMEM((T, D), BF16),
            pltpu.VMEM((Db,), F32),
            pltpu.VMEM((Fb,), F32),
            pltpu.VMEM((R, T, Fb), BF16),
            pltpu.VMEM((T, L * F2), F32),
            pltpu.VMEM((Db, 1), F32),
            pltpu.VMEM((plane * T, Fb), BF16),
            pltpu.VMEM((F2p, Fb), BF16),
            pltpu.VMEM((texts, L * F2), BF16),
            pltpu.VMEM((plane * T, F2p), F32),
            pltpu.VMEM((X, L * T, F2p), F32),
            pltpu.VMEM((X, L * T, F2p), F32),
            pltpu.VMEM((X, L, T, F2p), F32),
            pltpu.VMEM((T, L * F2), F32),
            pltpu.VMEM((2 * T, L * F2), BF16),
            pltpu.VMEM((T, L * F2), F32),
            pltpu.VMEM((T, L * F2), F32),
            pltpu.VMEM((L, T, F2), BF16),
            pltpu.VMEM((plane * T, F2), BF16),
            pltpu.VMEM((F2, plane * T), BF16),
            pltpu.VMEM((Z, Dp, Fb), F32),
            pltpu.VMEM((Z, Dp, Fb), BF16),
            pltpu.VMEM((2, Z, Dp, Fb), BF16),
            pltpu.VMEM((R, Db, 1), F32),
            pltpu.VMEM((C, 1, Fb), F32),
            pltpu.VMEM((R * C, 1, 128), F32),
            dma(6),
            one, one, one, dma(2, Z), dma(Z), dma(2, Z), one, dma(X * C), one, dma(2),
            one, dma(X, 2), one, dma(2), dma(2), dma(2),
            one, dma(plane), one, dma(2, Z, K), one, one, one, one, one, one,
        ],
        compiler_params=pltpu.CompilerParams(
            has_side_effects=True, collective_id=0, vmem_limit_bytes=60 * 1024 * 1024
        ),
    )(
        hidden, weight, pooled, text, row_moment, col_moment, log_scale[None], bias[None],
    )
    return upd, nr, nc, loss[0]


def solution(mesh):
    return jax.shard_map(
        per_device,
        mesh=mesh,
        in_specs=(
            P(("row", "col"), None),
            P(("row", "col"), None),
            P(("row", "col"), None),
            P("col", "row"),
            P("col"),
            P("row"),
            P(),
            P(),
        ),
        out_specs=(P("col", "row"), P("col"), P("row"), P()),
        check_vma=False,
    )
```

```python
import functools

import jax
import jax.numpy as jnp
from jax import lax
from jax.experimental import pallas as pl
from jax.experimental.pallas import tpu as pltpu
from jax.sharding import PartitionSpec as P

EPSILON = 1e-06
DECAY_RATE = 0.8
CLIP_LEVEL = 1.0
FLOOR_VALUE = 1e-30
CORES = 2
LOW = 2
MESH = pl.DeviceIdType.MESH
F32 = jnp.float32
BF16 = jnp.bfloat16


def dot_nt(a, b):
    return lax.dot_general(a, b, (((1,), (1,)), ((), ())), preferred_element_type=F32)


def kernel(
    sizes,
    hid_in, w_in, pool_in, text_in, rm_in, cm_in, ls_ref, bias_ref,
    upd_ref, nr_ref, nc_ref, loss_ref,
    hv, wv, pv, tv, rmv, cmv, hs, pool, rmc,
    hid, wg, txa, part, pre, summed, proj, mix, imgs, ug_s, ug_r, mg_s, mga, turned, gp, gz_s, gz,
    rsb, csb, stb, qcb, srb, hid2, mgx_s, mgx, ld,
    hid_ss, hid_rs, hx_rs, w_ss, w_rs, tz_ss, tp_ss, t_rs, td_ss, td_rs, pp_ss, pp_rs, p_ss, p_rs, pair_ss, pair_rs,
    mg_ss, mg_rs, g_ss, g_rs, row_ss, row_rs, col_ss, col_rs, st_ss, st_rs,
    qc_ss, qc_rs, sr_ss, sr_rs, hf_ss, hf_rs, mgx_ss, mgx_rs,
):
    R, C, X, Z, T, Db, Dp, Fb, K, E, F2, F2p, Fw = sizes
    L = LOW
    plane = R * L
    devices = R * C
    batch = devices * T
    r = lax.axis_index("row")
    c = lax.axis_index("col")
    z, y = c // L, c % L
    x, core = r // CORES, r % CORES
    q = r * L + y
    finish = []
    me = r * C + c
    Dc = Dp // K

    loads = [
        pltpu.make_async_copy(src, dst, ld.at[i])
        for i, (src, dst) in enumerate(
            ((w_in, wv), (hid_in, hv), (text_in, tv), (pool_in, pv), (rm_in, rmv), (cm_in, cmv))
        )
    ]
    for load in loads:
        load.start()
    barrier = pltpu.get_barrier_semaphore()

    def greet(device):
        pl.semaphore_signal(barrier, inc=1, device_id=device, device_id_type=MESH)

    for o in range(1, plane):
        other = lax.rem(q + o, plane)
        greet((other // L, z * L + other % L))
    pl.when(z > 0)(lambda: greet((r, c - L)))
    pl.when(z < Z - 1)(lambda: greet((r, c + L)))

    def send(src, dst, ss, rs, device, cond=None, bulk=False):
        def make():
            return pltpu.make_async_remote_copy(
                src_ref=src, dst_ref=dst, send_sem=ss, recv_sem=rs,
                device_id=device, device_id_type=MESH,
            )

        if cond is None:
            make().start()
        else:
            pl.when(cond)(lambda: make().start())
        if bulk:
            return
        if cond is None:
            finish.append(lambda: make().wait_send())
        else:
            finish.append(lambda: pl.when(cond)(lambda: make().wait_send()))

    def sent(like, ss):
        finish.append(lambda: pltpu.make_async_copy(like, like, ss).wait())

    def arrived(slot, rs):
        pltpu.make_async_copy(slot, slot, rs).wait()

    def rows(index, count):
        return pl.ds(pl.multiple_of(index * count, count), count)

    def by_half(value, store):
        for h in range(L):
            for k in range(Z):
                at = (k * L + h) * Db
                store(h * F2 + k * Dp, value[:, at:at + Db])

    own_slot = (z * X + x) * L + y
    loads[0].wait()
    if Dp != Db:
        wg[rows(z, Dp)] = jnp.zeros((Dp, Fb), BF16)
        txa[rows(own_slot, T)] = jnp.zeros((T, L * F2), BF16)
        pool[...] = jnp.zeros(pool.shape, F32)
    wg[pl.ds(pl.multiple_of(z * Dp, Dp), Db)] = wv[...].astype(BF16)
    if F2p != F2:
        wg[F2:F2p] = jnp.zeros((F2p - F2, Fb), BF16)
    loads[1].wait()
    for k in range(R):
        hs[k] = hv[:, k * Fb:(k + 1) * Fb]
    hid[rows(q, T)] = hs[r]
    loads[2].wait()
    tf = tv[...].astype(F32)
    tn = tf / jnp.sqrt(jnp.sum(tf * tf, axis=1, keepdims=True) + EPSILON)

    def put_text(at, value):
        txa[rows(own_slot, T), at:at + Db] = value.astype(BF16)

    by_half(tn, put_text)
    pl.semaphore_wait(barrier, plane - 1 + jnp.where(z > 0, 1, 0) + jnp.where(z < Z - 1, 1, 0))
    across = [lax.rem(x + o, X) for o in range(1, X)]
    beside = [lax.rem(y + o, L) for o in range(1, L)]
    partner = (x * CORES + (1 - core), c)
    own_rows = hid.at[rows(q, T)]
    for x2 in across:
        for k in range(CORES):
            r2 = x2 * CORES + k
            send(hs.at[r2], own_rows, hid_ss, hx_rs, (r2, c), bulk=True)
    for y2 in beside:
        for k in range(CORES):
            r2 = x * CORES + k
            send(hs.at[r2], own_rows, hid_ss, hid_rs, (r2, z * L + y2), bulk=True)
    send(hs.at[partner[0]], own_rows, hid_ss, hid_rs, partner, bulk=True)
    crossing = (X - 1) * CORES
    relayed = crossing * (L - 1)
    direct = crossing + CORES * (L - 1) + 1

    def hidden_on():
        arrived(hid.at[pl.ds(0, crossing * T)], hx_rs)
        for x2 in across:
            for k in range(CORES):
                at = hid.at[rows((x2 * CORES + k) * L + y, T)]
                for y2 in beside:
                    send(at, at, hid_ss, hid_rs, (r, z * L + y2), bulk=True)
        sent(hid.at[pl.ds(0, (direct + relayed) * T)], hid_ss)

    def text_place(zs):
        return (zs * X + x) * L + y

    def neighbours():
        along_x = [(lax.rem(x + o, X), y) for o in range(1, X)]
        return along_x + [(x, lax.rem(y + o, L)) for o in range(1, L)]

    split = T // 4
    low = z < Z // 2
    final = jnp.where(low, Z - 1, 0)
    edge = jnp.logical_and(E > 0, jnp.logical_or(z == 0, z == Z - 1))
    nearby = jnp.logical_and(E > 0, jnp.logical_or(z == 1, z == Z - 2))
    nest = jnp.where(low, 1, Z - 2)

    def relay(s):
        for d, direction in enumerate((1, -1)):
            if s == 0 and d:
                continue
            zs = z - direction * s
            has = jnp.logical_and(zs >= 0, zs < Z)
            block = jnp.clip(zs, 0, Z - 1)
            for n, (x2, y2) in enumerate(neighbours()):
                place = (block * X + x2) * L + y2
                at = txa.at[rows(place, T)]
                if s:
                    pl.when(has)(lambda: arrived(at, t_rs.at[place]))
                else:
                    arrived(at, t_rs.at[place])
                h = 0 if n < X - 1 else 1
                part_at = pl.multiple_of(place * T + h * split, split)
                half = txa.at[pl.ds(part_at, T - split if h else split)]
                onward = neighbours()[X - 1:] if h == 0 else neighbours()[:X - 1]
                for x3, y3 in onward:
                    send(
                        half, half, td_ss, td_rs,
                        (x3 * CORES + core, z * L + y3), has if s else None, True,
                    )

    def texts_on(s):
        for d, direction in enumerate((1, -1)):
            zs = z - direction * s
            nz = z + direction
            has = jnp.logical_and(zs >= 0, zs < Z)
            go = jnp.logical_and(has, jnp.logical_and(nz >= 0, nz < Z))
            place = text_place(jnp.clip(zs, 0, Z - 1))
            at = txa.at[rows(place, T)]
            if s:
                pl.when(has)(lambda: arrived(at, t_rs.at[place]))
            send(at, at, tz_ss.at[d, s], t_rs.at[place], (r, jnp.clip(nz, 0, Z - 1) * L + y), go)
            if s or d == 0:
                for x2, y2 in neighbours():
                    send(
                        at, at, tp_ss, t_rs.at[place],
                        (x2 * CORES + core, z * L + y2), has if s else None, True,
                    )

    def weights_on(s):
        for d, direction in enumerate((1, -1)):
            zs = z - direction * s
            nz = z + direction
            has = jnp.logical_and(zs >= 0, zs < Z)
            go = jnp.logical_and(has, jnp.logical_and(nz >= 0, nz < Z))
            block = jnp.clip(zs, 0, Z - 1)
            at = wg.at[rows(block, Dp)]
            if s:
                pl.when(has)(lambda: arrived(at, w_rs.at[block]))
            send(at, at, w_ss.at[d, s], w_rs.at[block], (r, jnp.clip(nz, 0, Z - 1) * L + y), go)

    texts_on(0)
    weights_on(0)
    loads[3].wait()

    def put_pool(at, value):
        pool[:, at:at + Db] = value

    by_half(pv[...].astype(F32), put_pool)
    loads[4].wait()
    loads[5].wait()
    eye = lax.broadcasted_iota(jnp.int32, (Db, Db), 0) == lax.broadcasted_iota(jnp.int32, (Db, Db), 1)
    line = jnp.broadcast_to(rmv[...].reshape(1, Db), (Db, Db))
    rmc[...] = jnp.sum(jnp.where(eye, line, 0.0), axis=1, keepdims=True)
    spans = (
        (pl.multiple_of(jnp.where(low, 0, Fw), 128), F2p - Fw),
        (pl.multiple_of(jnp.where(low, F2p - Fw, 0), 128), Fw),
    )

    def project(g):
        start, width = spans[g]
        lanes = pl.ds(start, width)
        part[:, lanes] = dot_nt(hid[...], wg[lanes])
        for o in range(1, X + 1):
            x2 = lax.rem(x + o, X)
            send(
                part.at[rows(x2 * CORES + 1 - core, L * T), lanes], pre.at[x2, :, lanes],
                pp_ss, pp_rs.at[x2, g], partner, bulk=True,
            )

    def spread(g):
        start, width = spans[g]
        lanes = pl.ds(start, width)
        for o in range(1, X + 1):
            x2 = lax.rem(x + o, X)
            arrived(pre.at[x2, :, lanes], pp_rs.at[x2, g])
            summed[x2, :, lanes] = part[rows(x2 * CORES + core, L * T), lanes] + pre[x2, :, lanes]
            for k in range(L):
                y2 = lax.rem(y + 1 + k, L)
                if o == X and k == L - 1:
                    proj[x, y, :, lanes] = summed[x, rows(y, T), lanes]
                else:
                    send(
                        summed.at[x2, rows(y2, T), lanes], proj.at[x, y, :, lanes], p_ss,
                        p_rs.at[g], (x2 * CORES + core, z * L + y2), bulk=True,
                    )

    def gathered(g):
        start, width = spans[g]
        arrived(part.at[pl.ds(0, (X * L - 1) * T), pl.ds(start, width)], p_rs.at[g])

    for s in range(1, Z):
        texts_on(s)
        if s == 1:
            hidden_on()
        if s == Z - 1:
            spread(0)
        else:
            weights_on(s)
        relay(s - 1)
        if s == Z - 2:
            arrived(hid.at[pl.ds(0, (plane - 1 - crossing) * T)], hid_rs)
            if E:
                send(hid, hid2, hf_ss, hf_rs, (r, nest * L + y), edge)
            project(0)
    weights_on(Z - 1)
    project(1)
    sent(part.at[pl.ds(0, X * L * T)], pp_ss)
    sent(part.at[pl.ds(0, (X * L - 1) * T)], p_ss)
    relay(Z - 1)
    spread(1)
    pairs_each = (X - 1) * (L - 1) * T
    sent(txa.at[pl.ds(0, Z * pairs_each)], td_ss)
    sent(txa.at[pl.ds(0, Z * (X + L - 2) * T)], tp_ss)
    gathered(0)
    gathered(1)
    for h in range(L):
        total = proj[0, h]
        for k in range(1, X):
            total = total + proj[k, h]
        mix[:, h * F2:(h + 1) * F2] = total[:, :F2]
    mixed = mix[...] + pool[...]
    length = jnp.sqrt(jnp.sum(mixed * mixed, axis=1, keepdims=True) + EPSILON)
    unit = mixed / length
    imgs[:T] = unit.astype(BF16)
    theirs = imgs.at[pl.ds(T, T)]
    send(imgs.at[pl.ds(0, T)], theirs, pair_ss.at[0], pair_rs.at[0], partner)
    scale = jnp.exp(jnp.full((1, 1), ls_ref[0], F32))
    bias = jnp.full((1, 1), bias_ref[0], F32)
    width = X * L * T

    def pairs(top, count, zs, blocks=1):
        images = imgs[top:top + count]
        texts = txa[pl.ds(pl.multiple_of(zs * width, width), blocks * width)]
        logits = scale * dot_nt(images, texts) + bias
        row_id = lax.broadcasted_iota(jnp.int32, logits.shape, 0) + top
        col_id = lax.broadcasted_iota(jnp.int32, logits.shape, 1) + (zs * width - own_slot * T)
        match = jnp.logical_and(row_id == col_id, row_id < T)
        u = jnp.where(match, -logits, logits)
        e = jnp.exp(-jnp.abs(u))
        loss = jnp.sum(jnp.maximum(u, 0.0) + jnp.log1p(e), axis=1, keepdims=True)
        sig = jnp.where(u >= 0, F32(1.0), e) / (1.0 + e)
        pg = (jnp.where(match, -sig, sig) / batch).astype(BF16)
        return loss, jnp.dot(pg, texts, preferred_element_type=F32)

    def more(k, carry):
        loss, grads = pairs(0, 2 * T, jnp.where(low, k, Z - 1 - k))
        return carry[0] + loss, carry[1] + grads

    arrived(txa.at[pl.ds(0, Z * pairs_each)], td_rs)
    arrived(theirs, pair_rs.at[0])
    carry = (jnp.zeros((2 * T, 1), F32), jnp.zeros((2 * T, L * F2), F32))
    tail = min(Z, 2)
    if Z <= 4:
        for k in range(Z - tail):
            carry = more(k, carry)
    else:
        carry = lax.fori_loop(0, Z - tail, more, carry)
    loss_most, grads = carry
    ending = jnp.where(low, Z - tail, 0)
    loss_b, grads_b = pairs(T, T, ending, tail)
    ug_s[...] = scale * (grads[T:] + grads_b)
    send(ug_s, ug_r, pair_ss.at[1], pair_rs.at[1], partner)
    loss_a, grads_a = pairs(0, T, ending, tail)
    arrived(ug_r, pair_rs.at[1])
    ug = scale * (grads[:T] + grads_a) + ug_r[...]
    inner = jnp.sum(unit * ug, axis=1, keepdims=True)
    mg = ((ug - unit * inner) / length).astype(BF16)
    for h in range(L):
        mg_s[h] = mg[:, h * F2:(h + 1) * F2]
    others = [
        (lax.rem(x + ox, X), lax.rem(y + oy, L))
        for ox in reversed(range(X)) for oy in reversed(range(L)) if ox or oy
    ]
    for x2, y2 in others:
        send(
            mg_s.at[y2], mga.at[rows(q, T)], mg_ss, mg_rs.at[q],
            (x2 * CORES + core, z * L + y2), bulk=True,
        )
    send(mg_s.at[y], mga.at[rows(q, T)], mg_ss, mg_rs.at[q], partner, bulk=True)
    mga[rows(q, T)] = mg_s[y]
    everyone = others + [(x, y)]
    if E:
        for h in range(L):
            top = mg[:, h * F2 + (Z - 1) * Dp:h * F2 + Z * Dp]
            mgx_s[h] = jnp.where(low, top, mg[:, h * F2:h * F2 + Dp])
        for x2, y2 in everyone:
            send(
                mgx_s.at[y2], mgx.at[rows(q, T)], mgx_ss, mgx_rs.at[q],
                (x2 * CORES + core, nest * L + y2), edge, True,
            )
    loss_local = jnp.sum(loss_a + loss_b, axis=0, keepdims=True) + jnp.sum(loss_most, axis=0, keepdims=True)
    stb[me] = jnp.broadcast_to(loss_local, (1, 128))

    def tell(o, _):
        other = lax.rem(me + o, devices)
        pltpu.make_async_remote_copy(
            src_ref=stb.at[me], dst_ref=stb.at[me], send_sem=st_ss, recv_sem=st_rs,
            device_id=(other // C, other % C), device_id_type=MESH,
        ).start()
        return _

    for x2, y2 in others:
        source = (x2 * CORES + core) * L + y2
        at = mga.at[rows(source, T)]
        arrived(at, mg_rs.at[source])
        send(at, at, mg_ss, mg_rs.at[source], partner, bulk=True)
    sent(mga.at[pl.ds(0, (plane - 1) * T)], mg_ss)
    if E:
        finish.append(lambda: pl.when(jnp.logical_or(edge, nearby))(
            lambda: arrived(mgx.at[pl.ds(0, X * L * T)], mgx_ss)
        ))
    for x2, y2 in [(x, y)] + others:
        source = (x2 * CORES + 1 - core) * L + y2
        arrived(mga.at[rows(source, T)], mg_rs.at[source])

    turned[...] = mga[...].T

    def own_part(zd):
        gp[zd] = jnp.dot(turned[rows(zd, Dp)], hid[...], preferred_element_type=F32)

    def far_part():
        for x2, y2 in everyone:
            at = mgx.at[rows((x2 * CORES + core) * L + y2, T)]
            arrived(at, mgx_rs.at[(x2 * CORES + core) * L + y2])
            send(at, at, mgx_ss, mgx_rs.at[(x2 * CORES + core) * L + y2], partner, bulk=True)
        arrived(hid2, hf_rs)
        for x2, y2 in everyone:
            source = (x2 * CORES + 1 - core) * L + y2
            arrived(mgx.at[rows(source, T)], mgx_rs.at[source])
        gp[final] = gp[final] + jnp.dot(mgx[...].T, hid2[...], preferred_element_type=F32)

    def pieces(tau, d):
        place = z if d == 0 else Z - 1 - z
        far = Z - 1 if d == 0 else 0
        i = tau - 2 * jnp.maximum(place - E, 0) + jnp.where(place == 0, K * E, 0)
        zd = jnp.clip(i, 0, Z * K - 1) // K
        k = jnp.clip(i, 0, Z * K - 1) % K
        zd = Z - 1 - zd if d == 0 else zd
        beyond = zd > z if d == 0 else zd < z
        ready = jnp.logical_and(i >= 0, i < Z * K)
        opens = jnp.logical_or(place == 0, jnp.logical_and(place == E, zd == far))
        return zd, k, jnp.logical_and(ready, beyond), jnp.logical_and(ready, zd == z), opens, place

    def step(tau, held):
        for d in range(2):
            zd, k, passing, ending, opens, place = pieces(tau, d)
            cut = rows(k, Dc)
            at = gz.at[d, zd, cut]
            copy = pltpu.make_async_remote_copy(
                src_ref=gz_s.at[zd, cut], dst_ref=at, send_sem=g_ss, recv_sem=g_rs.at[d, zd, k],
                device_id=(r, jnp.clip(z + (1 if d == 0 else -1), 0, Z - 1) * L + y), device_id_type=MESH,
            )

            def first():
                gz_s[zd, cut] = gp[zd, cut].astype(BF16)
                copy.start()

            def onward():
                arrived(at, g_rs.at[d, zd, k])
                gz_s[zd, cut] = (gp[zd, cut] + at[...].astype(F32)).astype(BF16)
                copy.start()

            def last():
                arrived(at, g_rs.at[d, zd, k])
                gp[zd, cut] = gp[zd, cut] + at[...].astype(F32)

            passing = jnp.logical_and(passing, held)
            ending = jnp.logical_and(jnp.logical_and(ending, held), place > 0)
            pl.when(jnp.logical_and(passing, opens))(first)
            pl.when(jnp.logical_and(passing, jnp.logical_not(opens)))(onward)
            pl.when(ending)(last)

    def early(tau, _):
        step(tau, edge)
        return _

    def later(tau, _):
        step(tau, jnp.logical_or(jnp.logical_not(edge), tau >= head))
        return _

    steps_g = max((Z - 1) * K + 1 - 2 * E, K - 1 + 2 * (Z - 1 - E)) + 1
    head = min(K, 2)

    def order(k):
        return jnp.where(low, Z - 1 - k, k)

    if E:
        own_part(order(1))
        lax.fori_loop(0, head, early, 0)
        pl.when(jnp.logical_not(edge))(lambda: own_part(order(0)))
        for k in range(2, Z):
            own_part(order(k))
        lax.fori_loop(1, devices, tell, 0)
        pl.when(nearby)(far_part)
        finish.append(lambda: pl.when(edge)(lambda: arrived(gz_s.at[pl.ds(0, Z - 2)], g_ss)))
        finish.append(lambda: pl.when(jnp.logical_not(edge))(lambda: arrived(gz_s.at[pl.ds(0, Z - 1)], g_ss)))
    else:
        for k in range(Z):
            own_part(order(k))
        lax.fori_loop(1, devices, tell, 0)
        sent(gz_s.at[pl.ds(0, Z - 1)], g_ss)
    lax.fori_loop(0, steps_g, later, 0)
    g = gp[z][:Db]

    def across_cols(box, ss, rs):
        for o in range(1, C):
            send(box.at[c], box.at[c], ss, rs, (r, lax.rem(c + o, C)), bulk=True)
        sent(box.at[pl.ds(0, C - 1)], ss)

    def across_rows(box, ss, rs, also=lambda: None):
        for o in range(1, R):
            send(box.at[r], box.at[r], ss, rs, (lax.rem(r + o, R), c), bulk=True)
        sent(box.at[pl.ds(0, R - 1)], ss)
        also()
        arrived(box.at[pl.ds(0, R - 1)], rs)

    square = g * g
    sq = square + FLOOR_VALUE
    rsb[r] = jnp.sum(jnp.where(eye, jnp.sum(sq, axis=1, keepdims=True), 0.0), axis=0, keepdims=True)
    csb[c] = jnp.sum(sq, axis=0, keepdims=True)
    across_rows(rsb, row_ss, row_rs, lambda: across_cols(csb, col_ss, col_rs))
    row_sum = jnp.broadcast_to(sum(rsb[k] for k in range(R)), (Db, Db))
    row_sum = jnp.sum(jnp.where(eye, row_sum, 0.0), axis=1, keepdims=True)
    new_row = DECAY_RATE * rmc[...] + (1.0 - DECAY_RATE) * row_sum / (R * Fb)
    qcb[c] = jnp.sum(square / new_row, axis=0, keepdims=True)
    across_cols(qcb, qc_ss, qc_rs)
    nr_ref[...] = jnp.sum(jnp.where(eye, new_row, 0.0), axis=0)
    arrived(csb.at[pl.ds(0, C - 1)], col_rs)
    col_sum = sum(csb[k] for k in range(C))
    new_col = DECAY_RATE * cmv[...].reshape(1, Fb) + (1.0 - DECAY_RATE) * col_sum / (C * Db)
    nc_ref[...] = new_col[0]
    upd_ref[...] = g / jnp.sqrt(new_row * new_col)
    arrived(qcb.at[pl.ds(0, C - 1)], qc_rs)
    part_sum = jnp.sum(sum(qcb[k] for k in range(C)) / new_col, axis=1, keepdims=True)
    srb[r] = jnp.broadcast_to(part_sum, (1, 128))
    across_rows(srb, sr_ss, sr_rs)
    total = sum(srb[k] for k in range(R))[:, 0:1]
    rms = jnp.sqrt(total / (C * Db * R * Fb))
    upd_ref[...] = upd_ref[...] / jnp.maximum(1.0, rms / CLIP_LEVEL)
    sent(stb.at[pl.ds(0, devices - 1)], st_ss)
    arrived(stb.at[pl.ds(0, devices - 1)], st_rs)
    lane = lax.broadcasted_iota(jnp.int32, (1, 128), 1)
    totals = jnp.sum(stb[...], axis=0)
    loss_ref[0] = jnp.sum(jnp.where(lane == 1, totals, 0.0)) / batch
    for wait in finish:
        wait()


def per_device(pooled, hidden, text, weight, row_moment, col_moment, log_scale, bias):
    R, C = lax.axis_size("row"), lax.axis_size("col")
    L, X, Z = LOW, R // CORES, C // LOW
    T, D = pooled.shape
    Db, Fb = weight.shape
    Dp = -(-Db // 16) * 16
    F2 = Z * Dp
    plane = R * L
    texts = X * C * T

    K = 3 if Dp % 48 == 0 else 1
    E = 1 if Z >= 4 else 0
    F2p = -(-F2 // 128) * 128
    Fw = max(-(-Dp // 128) * 128, F2p - (F2 - Dp) // 128 * 128)
    sizes = (R, C, X, Z, T, Db, Dp, Fb, K, E, F2, F2p, Fw)
    vmem = pl.BlockSpec(memory_space=pltpu.VMEM)
    smem = pl.BlockSpec(memory_space=pltpu.SMEM)
    dma = lambda *s: pltpu.SemaphoreType.DMA(s)
    one = pltpu.SemaphoreType.DMA
    upd, nr, nc, loss = pl.pallas_call(
        functools.partial(kernel, sizes),
        out_shape=(
            jax.ShapeDtypeStruct((Db, Fb), F32),
            jax.ShapeDtypeStruct((Db,), F32),
            jax.ShapeDtypeStruct((Fb,), F32),
            jax.ShapeDtypeStruct((1,), F32),
        ),
        in_specs=[pl.BlockSpec(memory_space=pl.ANY)] * 6 + [smem] * 2,
        out_specs=(vmem,) * 3 + (smem,),
        scratch_shapes=[
            pltpu.VMEM((T, R * Fb), BF16),
            pltpu.VMEM((Db, Fb), F32),
            pltpu.VMEM((T, D), BF16),
            pltpu.VMEM((T, D), BF16),
            pltpu.VMEM((Db,), F32),
            pltpu.VMEM((Fb,), F32),
            pltpu.VMEM((R, T, Fb), BF16),
            pltpu.VMEM((T, L * F2), F32),
            pltpu.VMEM((Db, 1), F32),
            pltpu.VMEM((plane * T, Fb), BF16),
            pltpu.VMEM((F2p, Fb), BF16),
            pltpu.VMEM((texts, L * F2), BF16),
            pltpu.VMEM((plane * T, F2p), F32),
            pltpu.VMEM((X, L * T, F2p), F32),
            pltpu.VMEM((X, L * T, F2p), F32),
            pltpu.VMEM((X, L, T, F2p), F32),
            pltpu.VMEM((T, L * F2), F32),
            pltpu.VMEM((2 * T, L * F2), BF16),
            pltpu.VMEM((T, L * F2), F32),
            pltpu.VMEM((T, L * F2), F32),
            pltpu.VMEM((L, T, F2), BF16),
            pltpu.VMEM((plane * T, F2), BF16),
            pltpu.VMEM((F2, plane * T), BF16),
            pltpu.VMEM((Z, Dp, Fb), F32),
            pltpu.VMEM((Z, Dp, Fb), BF16),
            pltpu.VMEM((2, Z, Dp, Fb), BF16),
            pltpu.VMEM((R, 1, Db), F32),
            pltpu.VMEM((C, 1, Fb), F32),
            pltpu.VMEM((R * C, 1, 128), F32),
            pltpu.VMEM((C, 1, Fb), F32),
            pltpu.VMEM((R, 1, 128), F32),
            pltpu.VMEM((plane * T, Fb), BF16),
            pltpu.VMEM((L, T, Dp), BF16),
            pltpu.VMEM((plane * T, Dp), BF16),
            dma(6),
            one, one, one, dma(2, Z), dma(Z), dma(2, Z), one, dma(X * C), one, one,
            one, dma(X, 2), one, dma(2), dma(2), dma(2),
            one, dma(plane), one, dma(2, Z, K), one, one, one, one, one, one,
            one, one, one, one, one, one, one, dma(plane),
        ],
        compiler_params=pltpu.CompilerParams(
            has_side_effects=True, collective_id=0, vmem_limit_bytes=60 * 1024 * 1024
        ),
    )(
        hidden, weight, pooled, text, row_moment, col_moment, log_scale[None], bias[None],
    )
    return upd, nr, nc, loss[0]


def solution(mesh):
    return jax.shard_map(
        per_device,
        mesh=mesh,
        in_specs=(
            P(("row", "col"), None),
            P(("row", "col"), None),
            P(("row", "col"), None),
            P("col", "row"),
            P("col"),
            P("row"),
            P(),
            P(),
        ),
        out_specs=(P("col", "row"), P("col"), P("row"), P()),
        check_vma=False,
    )
```

```python
import functools

import jax
import jax.numpy as jnp
from jax import lax
from jax.experimental import pallas as pl
from jax.experimental.pallas import tpu as pltpu
from jax.sharding import PartitionSpec as P

EPSILON = 1e-06
DECAY_RATE = 0.8
CLIP_LEVEL = 1.0
FLOOR_VALUE = 1e-30
CORES = 2
LOW = 2
MESH = pl.DeviceIdType.MESH
F32 = jnp.float32
BF16 = jnp.bfloat16


def dot_nt(a, b):
    return lax.dot_general(a, b, (((1,), (1,)), ((), ())), preferred_element_type=F32)


def kernel(
    sizes,
    hid_in, w_in, pool_in, text_in, rm_in, cm_in, ls_ref, bias_ref,
    upd_out, nr_out, nc_out, end_ref,
    hv, wv, pv, tv, rmv, cmv, hs, pool, rmc,
    hid, wg, txa, part, pre, summed, proj, mix, imgs, ug_s, ug_r, mg_s, mga, turned, gp, gz_s, gz,
    upd_ref, nr_ref, nc_ref, rsb, csb, stb, qcb, srb, hid2, mgx_s, mgx, ld,
    hid_ss, hid_rs, hx_rs, w_ss, w_rs, tz_ss, tp_ss, t_rs, td_ss, td_rs, pp_ss, pp_rs, p_ss, p_rs, pair_ss, pair_rs,
    mg_ss, mg_rs, g_ss, g_rs, row_ss, row_rs, col_ss, col_rs, st_ss, st_rs,
    qc_ss, qc_rs, sr_ss, sr_rs, hf_ss, hf_rs, mgx_ss, mgx_rs,
):
    R, C, X, Z, T, Db, Dp, Fb, K, E, F2, F2p, Fw = sizes
    L = LOW
    plane = R * L
    devices = R * C
    batch = devices * T
    r = lax.axis_index("row")
    c = lax.axis_index("col")
    z, y = c // L, c % L
    x, core = r // CORES, r % CORES
    q = r * L + y
    finish = []
    me = r * C + c
    Dc = Dp // K

    loads = [
        pltpu.make_async_copy(src, dst, ld.at[i])
        for i, (src, dst) in enumerate(
            ((w_in, wv), (hid_in, hv), (text_in, tv), (pool_in, pv), (rm_in, rmv), (cm_in, cmv))
        )
    ]
    for load in loads:
        load.start()
    barrier = pltpu.get_barrier_semaphore()

    def greet(device):
        pl.semaphore_signal(barrier, inc=1, device_id=device, device_id_type=MESH)

    for o in range(1, plane):
        other = lax.rem(q + o, plane)
        greet((other // L, z * L + other % L))
    pl.when(z > 0)(lambda: greet((r, c - L)))
    pl.when(z < Z - 1)(lambda: greet((r, c + L)))

    def send(src, dst, ss, rs, device, cond=None, bulk=False):
        def make():
            return pltpu.make_async_remote_copy(
                src_ref=src, dst_ref=dst, send_sem=ss, recv_sem=rs,
                device_id=device, device_id_type=MESH,
            )

        if cond is None:
            make().start()
        else:
            pl.when(cond)(lambda: make().start())
        if bulk:
            return
        if cond is None:
            finish.append(lambda: make().wait_send())
        else:
            finish.append(lambda: pl.when(cond)(lambda: make().wait_send()))

    def sent(like, ss):
        finish.append(lambda: pltpu.make_async_copy(like, like, ss).wait())

    def arrived(slot, rs):
        pltpu.make_async_copy(slot, slot, rs).wait()

    def rows(index, count):
        return pl.ds(pl.multiple_of(index * count, count), count)

    def by_half(value, store):
        for h in range(L):
            for k in range(Z):
                at = (k * L + h) * Db
                store(h * F2 + k * Dp, value[:, at:at + Db])

    own_slot = (z * X + x) * L + y
    loads[0].wait()
    if Dp != Db:
        wg[rows(z, Dp)] = jnp.zeros((Dp, Fb), BF16)
        txa[rows(own_slot, T)] = jnp.zeros((T, L * F2), BF16)
        pool[...] = jnp.zeros(pool.shape, F32)
    wg[pl.ds(pl.multiple_of(z * Dp, Dp), Db)] = wv[...].astype(BF16)
    if F2p != F2:
        wg[F2:F2p] = jnp.zeros((F2p - F2, Fb), BF16)
    loads[1].wait()
    for k in range(R):
        hs[k] = hv[:, k * Fb:(k + 1) * Fb]
    hid[rows(q, T)] = hs[r]
    loads[2].wait()
    tf = tv[...].astype(F32)
    tn = tf / jnp.sqrt(jnp.sum(tf * tf, axis=1, keepdims=True) + EPSILON)

    def put_text(at, value):
        txa[rows(own_slot, T), at:at + Db] = value.astype(BF16)

    by_half(tn, put_text)
    pl.semaphore_wait(barrier, plane - 1 + jnp.where(z > 0, 1, 0) + jnp.where(z < Z - 1, 1, 0))
    across = [lax.rem(x + o, X) for o in range(1, X)]
    beside = [lax.rem(y + o, L) for o in range(1, L)]
    partner = (x * CORES + (1 - core), c)
    own_rows = hid.at[rows(q, T)]
    for x2 in across:
        for k in range(CORES):
            r2 = x2 * CORES + k
            send(hs.at[r2], own_rows, hid_ss, hx_rs, (r2, c), bulk=True)
    for y2 in beside:
        for k in range(CORES):
            r2 = x * CORES + k
            send(hs.at[r2], own_rows, hid_ss, hid_rs, (r2, z * L + y2), bulk=True)
    send(hs.at[partner[0]], own_rows, hid_ss, hid_rs, partner, bulk=True)
    crossing = (X - 1) * CORES
    relayed = crossing * (L - 1)
    direct = crossing + CORES * (L - 1) + 1

    def hidden_on():
        arrived(hid.at[pl.ds(0, crossing * T)], hx_rs)
        for x2 in across:
            for k in range(CORES):
                at = hid.at[rows((x2 * CORES + k) * L + y, T)]
                for y2 in beside:
                    send(at, at, hid_ss, hid_rs, (r, z * L + y2), bulk=True)
        sent(hid.at[pl.ds(0, (direct + relayed) * T)], hid_ss)

    def text_place(zs):
        return (zs * X + x) * L + y

    def neighbours():
        along_x = [(lax.rem(x + o, X), y) for o in range(1, X)]
        return along_x + [(x, lax.rem(y + o, L)) for o in range(1, L)]

    split = T // 4
    low = z < Z // 2
    final = jnp.where(low, Z - 1, 0)
    edge = jnp.logical_and(E > 0, jnp.logical_or(z == 0, z == Z - 1))
    nearby = jnp.logical_and(E > 0, jnp.logical_or(z == 1, z == Z - 2))
    nest = jnp.where(low, 1, Z - 2)

    def relay(s):
        for d, direction in enumerate((1, -1)):
            if s == 0 and d:
                continue
            zs = z - direction * s
            has = jnp.logical_and(zs >= 0, zs < Z)
            block = jnp.clip(zs, 0, Z - 1)
            for n, (x2, y2) in enumerate(neighbours()):
                place = (block * X + x2) * L + y2
                at = txa.at[rows(place, T)]
                if s:
                    pl.when(has)(lambda: arrived(at, t_rs.at[place]))
                else:
                    arrived(at, t_rs.at[place])
                h = 0 if n < X - 1 else 1
                part_at = pl.multiple_of(place * T + h * split, split)
                half = txa.at[pl.ds(part_at, T - split if h else split)]
                onward = neighbours()[X - 1:] if h == 0 else neighbours()[:X - 1]
                for x3, y3 in onward:
                    send(
                        half, half, td_ss, td_rs,
                        (x3 * CORES + core, z * L + y3), has if s else None, True,
                    )

    def texts_on(s):
        for d, direction in enumerate((1, -1)):
            zs = z - direction * s
            nz = z + direction
            has = jnp.logical_and(zs >= 0, zs < Z)
            go = jnp.logical_and(has, jnp.logical_and(nz >= 0, nz < Z))
            place = text_place(jnp.clip(zs, 0, Z - 1))
            at = txa.at[rows(place, T)]
            if s:
                pl.when(has)(lambda: arrived(at, t_rs.at[place]))
            send(at, at, tz_ss.at[d, s], t_rs.at[place], (r, jnp.clip(nz, 0, Z - 1) * L + y), go)
            if s or d == 0:
                for x2, y2 in neighbours():
                    send(
                        at, at, tp_ss, t_rs.at[place],
                        (x2 * CORES + core, z * L + y2), has if s else None, True,
                    )

    def weights_on(s):
        for d, direction in enumerate((1, -1)):
            zs = z - direction * s
            nz = z + direction
            has = jnp.logical_and(zs >= 0, zs < Z)
            go = jnp.logical_and(has, jnp.logical_and(nz >= 0, nz < Z))
            block = jnp.clip(zs, 0, Z - 1)
            at = wg.at[rows(block, Dp)]
            if s:
                pl.when(has)(lambda: arrived(at, w_rs.at[block]))
            send(at, at, w_ss.at[d, s], w_rs.at[block], (r, jnp.clip(nz, 0, Z - 1) * L + y), go)

    texts_on(0)
    weights_on(0)
    loads[3].wait()

    def put_pool(at, value):
        pool[:, at:at + Db] = value

    by_half(pv[...].astype(F32), put_pool)
    loads[4].wait()
    loads[5].wait()
    eye = lax.broadcasted_iota(jnp.int32, (Db, Db), 0) == lax.broadcasted_iota(jnp.int32, (Db, Db), 1)
    line = jnp.broadcast_to(rmv[...].reshape(1, Db), (Db, Db))
    rmc[...] = jnp.sum(jnp.where(eye, line, 0.0), axis=1, keepdims=True)
    spans = (
        (pl.multiple_of(jnp.where(low, 0, Fw), 128), F2p - Fw),
        (pl.multiple_of(jnp.where(low, F2p - Fw, 0), 128), Fw),
    )

    def project(g):
        start, width = spans[g]
        lanes = pl.ds(start, width)
        part[:, lanes] = dot_nt(hid[...], wg[lanes])
        for o in range(1, X + 1):
            x2 = lax.rem(x + o, X)
            send(
                part.at[rows(x2 * CORES + 1 - core, L * T), lanes], pre.at[x2, :, lanes],
                pp_ss, pp_rs.at[x2, g], partner, bulk=True,
            )

    def spread(g):
        start, width = spans[g]
        lanes = pl.ds(start, width)
        for o in range(1, X + 1):
            x2 = lax.rem(x + o, X)
            arrived(pre.at[x2, :, lanes], pp_rs.at[x2, g])
            summed[x2, :, lanes] = part[rows(x2 * CORES + core, L * T), lanes] + pre[x2, :, lanes]
            for k in range(L):
                y2 = lax.rem(y + 1 + k, L)
                if o == X and k == L - 1:
                    proj[x, y, :, lanes] = summed[x, rows(y, T), lanes]
                else:
                    send(
                        summed.at[x2, rows(y2, T), lanes], proj.at[x, y, :, lanes], p_ss,
                        p_rs.at[g], (x2 * CORES + core, z * L + y2), bulk=True,
                    )

    def gathered(g):
        start, width = spans[g]
        arrived(part.at[pl.ds(0, (X * L - 1) * T), pl.ds(start, width)], p_rs.at[g])

    for s in range(1, Z):
        texts_on(s)
        if s == 1:
            hidden_on()
        if s == Z - 1:
            spread(0)
        else:
            weights_on(s)
        relay(s - 1)
        if s == Z - 2:
            arrived(hid.at[pl.ds(0, (plane - 1 - crossing) * T)], hid_rs)
            if E:
                send(hid, hid2, hf_ss, hf_rs, (r, nest * L + y), edge)
            project(0)
    weights_on(Z - 1)
    project(1)
    sent(part.at[pl.ds(0, X * L * T)], pp_ss)
    sent(part.at[pl.ds(0, (X * L - 1) * T)], p_ss)
    relay(Z - 1)
    spread(1)
    pairs_each = (X - 1) * (L - 1) * T
    sent(txa.at[pl.ds(0, Z * pairs_each)], td_ss)
    sent(txa.at[pl.ds(0, Z * (X + L - 2) * T)], tp_ss)
    gathered(0)
    gathered(1)
    for h in range(L):
        total = proj[0, h]
        for k in range(1, X):
            total = total + proj[k, h]
        mix[:, h * F2:(h + 1) * F2] = total[:, :F2]
    mixed = mix[...] + pool[...]
    length = jnp.sqrt(jnp.sum(mixed * mixed, axis=1, keepdims=True) + EPSILON)
    unit = mixed / length
    imgs[:T] = unit.astype(BF16)
    theirs = imgs.at[pl.ds(T, T)]
    send(imgs.at[pl.ds(0, T)], theirs, pair_ss.at[0], pair_rs.at[0], partner)
    scale = jnp.exp(jnp.full((1, 1), ls_ref[0], F32))
    bias = jnp.full((1, 1), bias_ref[0], F32)
    width = X * L * T

    def pairs(top, count, zs, blocks=1):
        images = imgs[top:top + count]
        texts = txa[pl.ds(pl.multiple_of(zs * width, width), blocks * width)]
        logits = scale * dot_nt(images, texts) + bias
        row_id = lax.broadcasted_iota(jnp.int32, logits.shape, 0) + top
        col_id = lax.broadcasted_iota(jnp.int32, logits.shape, 1) + (zs * width - own_slot * T)
        match = jnp.logical_and(row_id == col_id, row_id < T)
        u = jnp.where(match, -logits, logits)
        e = jnp.exp(-jnp.abs(u))
        loss = jnp.sum(jnp.maximum(u, 0.0) + jnp.log1p(e), axis=1, keepdims=True)
        sig = jnp.where(u >= 0, F32(1.0), e) / (1.0 + e)
        pg = (jnp.where(match, -sig, sig) / batch).astype(BF16)
        return loss, jnp.dot(pg, texts, preferred_element_type=F32)

    def more(k, carry):
        loss, grads = pairs(0, 2 * T, jnp.where(low, k, Z - 1 - k))
        return carry[0] + loss, carry[1] + grads

    arrived(txa.at[pl.ds(0, Z * pairs_each)], td_rs)
    arrived(theirs, pair_rs.at[0])
    carry = (jnp.zeros((2 * T, 1), F32), jnp.zeros((2 * T, L * F2), F32))
    tail = min(Z, 2)
    if Z <= 4:
        for k in range(Z - tail):
            carry = more(k, carry)
    else:
        carry = lax.fori_loop(0, Z - tail, more, carry)
    loss_most, grads = carry
    ending = jnp.where(low, Z - tail, 0)
    loss_b, grads_b = pairs(T, T, ending, tail)
    ug_s[...] = scale * (grads[T:] + grads_b)
    send(ug_s, ug_r, pair_ss.at[1], pair_rs.at[1], partner)
    loss_a, grads_a = pairs(0, T, ending, tail)
    arrived(ug_r, pair_rs.at[1])
    ug = scale * (grads[:T] + grads_a) + ug_r[...]
    inner = jnp.sum(unit * ug, axis=1, keepdims=True)
    mg = ((ug - unit * inner) / length).astype(BF16)
    for h in range(L):
        mg_s[h] = mg[:, h * F2:(h + 1) * F2]
    others = [
        (lax.rem(x + ox, X), lax.rem(y + oy, L))
        for ox in reversed(range(X)) for oy in reversed(range(L)) if ox or oy
    ]
    for x2, y2 in others:
        send(
            mg_s.at[y2], mga.at[rows(q, T)], mg_ss, mg_rs.at[q],
            (x2 * CORES + core, z * L + y2), bulk=True,
        )
    send(mg_s.at[y], mga.at[rows(q, T)], mg_ss, mg_rs.at[q], partner, bulk=True)
    mga[rows(q, T)] = mg_s[y]
    everyone = others + [(x, y)]
    if E:
        for h in range(L):
            top = mg[:, h * F2 + (Z - 1) * Dp:h * F2 + Z * Dp]
            mgx_s[h] = jnp.where(low, top, mg[:, h * F2:h * F2 + Dp])
        for x2, y2 in everyone:
            send(
                mgx_s.at[y2], mgx.at[rows(q, T)], mgx_ss, mgx_rs.at[q],
                (x2 * CORES + core, nest * L + y2), edge, True,
            )
    loss_local = jnp.sum(loss_a + loss_b, axis=0, keepdims=True) + jnp.sum(loss_most, axis=0, keepdims=True)
    stb[me] = jnp.broadcast_to(loss_local, (1, 128))

    def tell(o, _):
        other = lax.rem(me + o, devices)
        pltpu.make_async_remote_copy(
            src_ref=stb.at[me], dst_ref=stb.at[me], send_sem=st_ss, recv_sem=st_rs,
            device_id=(other // C, other % C), device_id_type=MESH,
        ).start()
        return _

    for x2, y2 in others:
        source = (x2 * CORES + core) * L + y2
        at = mga.at[rows(source, T)]
        arrived(at, mg_rs.at[source])
        send(at, at, mg_ss, mg_rs.at[source], partner, bulk=True)
    sent(mga.at[pl.ds(0, (plane - 1) * T)], mg_ss)
    if E:
        finish.append(lambda: pl.when(jnp.logical_or(edge, nearby))(
            lambda: arrived(mgx.at[pl.ds(0, X * L * T)], mgx_ss)
        ))
    for x2, y2 in [(x, y)] + others:
        source = (x2 * CORES + 1 - core) * L + y2
        arrived(mga.at[rows(source, T)], mg_rs.at[source])

    turned[...] = mga[...].T

    def own_part(zd):
        gp[zd] = jnp.dot(turned[rows(zd, Dp)], hid[...], preferred_element_type=F32)

    def far_part():
        for x2, y2 in everyone:
            at = mgx.at[rows((x2 * CORES + core) * L + y2, T)]
            arrived(at, mgx_rs.at[(x2 * CORES + core) * L + y2])
            send(at, at, mgx_ss, mgx_rs.at[(x2 * CORES + core) * L + y2], partner, bulk=True)
        arrived(hid2, hf_rs)
        for x2, y2 in everyone:
            source = (x2 * CORES + 1 - core) * L + y2
            arrived(mgx.at[rows(source, T)], mgx_rs.at[source])
        gp[final] = gp[final] + jnp.dot(mgx[...].T, hid2[...], preferred_element_type=F32)

    def pieces(tau, d):
        place = z if d == 0 else Z - 1 - z
        far = Z - 1 if d == 0 else 0
        i = tau - 2 * jnp.maximum(place - E, 0) + jnp.where(place == 0, K * E, 0)
        zd = jnp.clip(i, 0, Z * K - 1) // K
        k = jnp.clip(i, 0, Z * K - 1) % K
        zd = Z - 1 - zd if d == 0 else zd
        beyond = zd > z if d == 0 else zd < z
        ready = jnp.logical_and(i >= 0, i < Z * K)
        opens = jnp.logical_or(place == 0, jnp.logical_and(place == E, zd == far))
        return zd, k, jnp.logical_and(ready, beyond), jnp.logical_and(ready, zd == z), opens, place

    def step(tau, held):
        for d in range(2):
            zd, k, passing, ending, opens, place = pieces(tau, d)
            cut = rows(k, Dc)
            at = gz.at[d, zd, cut]
            copy = pltpu.make_async_remote_copy(
                src_ref=gz_s.at[zd, cut], dst_ref=at, send_sem=g_ss, recv_sem=g_rs.at[d, zd, k],
                device_id=(r, jnp.clip(z + (1 if d == 0 else -1), 0, Z - 1) * L + y), device_id_type=MESH,
            )

            def first():
                gz_s[zd, cut] = gp[zd, cut].astype(BF16)
                copy.start()

            def onward():
                arrived(at, g_rs.at[d, zd, k])
                gz_s[zd, cut] = (gp[zd, cut] + at[...].astype(F32)).astype(BF16)
                copy.start()

            def last():
                arrived(at, g_rs.at[d, zd, k])
                gp[zd, cut] = gp[zd, cut] + at[...].astype(F32)

            passing = jnp.logical_and(passing, held)
            ending = jnp.logical_and(jnp.logical_and(ending, held), place > 0)
            pl.when(jnp.logical_and(passing, opens))(first)
            pl.when(jnp.logical_and(passing, jnp.logical_not(opens)))(onward)
            pl.when(ending)(last)

    def early(tau, _):
        step(tau, edge)
        return _

    def later(tau, _):
        step(tau, jnp.logical_or(jnp.logical_not(edge), tau >= head))
        return _

    steps_g = max((Z - 1) * K + 1 - 2 * E, K - 1 + 2 * (Z - 1 - E)) + 1
    head = min(K, 2)

    def order(k):
        return jnp.where(low, Z - 1 - k, k)

    if E:
        own_part(order(1))
        lax.fori_loop(0, head, early, 0)
        pl.when(jnp.logical_not(edge))(lambda: own_part(order(0)))
        for k in range(2, Z):
            own_part(order(k))
        lax.fori_loop(1, devices, tell, 0)
        pl.when(nearby)(far_part)
        finish.append(lambda: pl.when(edge)(lambda: arrived(gz_s.at[pl.ds(0, Z - 2)], g_ss)))
        finish.append(lambda: pl.when(jnp.logical_not(edge))(lambda: arrived(gz_s.at[pl.ds(0, Z - 1)], g_ss)))
    else:
        for k in range(Z):
            own_part(order(k))
        lax.fori_loop(1, devices, tell, 0)
        sent(gz_s.at[pl.ds(0, Z - 1)], g_ss)
    lax.fori_loop(0, steps_g, later, 0)
    g = gp[z][:Db]

    def across_cols(box, ss, rs):
        for o in range(1, C):
            send(box.at[c], box.at[c], ss, rs, (r, lax.rem(c + o, C)), bulk=True)
        sent(box.at[pl.ds(0, C - 1)], ss)

    def across_rows(box, ss, rs, also=lambda: None):
        for o in range(1, R):
            send(box.at[r], box.at[r], ss, rs, (lax.rem(r + o, R), c), bulk=True)
        sent(box.at[pl.ds(0, R - 1)], ss)
        also()
        arrived(box.at[pl.ds(0, R - 1)], rs)

    square = g * g
    sq = square + FLOOR_VALUE
    rsb[r] = jnp.sum(jnp.where(eye, jnp.sum(sq, axis=1, keepdims=True), 0.0), axis=0, keepdims=True)
    csb[c] = jnp.sum(sq, axis=0, keepdims=True)
    across_rows(rsb, row_ss, row_rs, lambda: across_cols(csb, col_ss, col_rs))
    row_sum = jnp.broadcast_to(sum(rsb[k] for k in range(R)), (Db, Db))
    row_sum = jnp.sum(jnp.where(eye, row_sum, 0.0), axis=1, keepdims=True)
    new_row = DECAY_RATE * rmc[...] + (1.0 - DECAY_RATE) * row_sum / (R * Fb)
    qcb[c] = jnp.sum(square / new_row, axis=0, keepdims=True)
    across_cols(qcb, qc_ss, qc_rs)
    nr_ref[...] = jnp.sum(jnp.where(eye, new_row, 0.0), axis=0)
    arrived(csb.at[pl.ds(0, C - 1)], col_rs)
    col_sum = sum(csb[k] for k in range(C))
    new_col = DECAY_RATE * cmv[...].reshape(1, Fb) + (1.0 - DECAY_RATE) * col_sum / (C * Db)
    nc_ref[...] = new_col[0]
    upd_ref[...] = g / jnp.sqrt(new_row * new_col)
    for i, (src, dst) in enumerate(((upd_ref, upd_out), (nr_ref, nr_out), (nc_ref, nc_out))):
        store = pltpu.make_async_copy(src, dst, ld.at[6 + i])
        store.start()
        finish.append(store.wait)
    arrived(qcb.at[pl.ds(0, C - 1)], qc_rs)
    part_sum = jnp.sum(sum(qcb[k] for k in range(C)) / new_col, axis=1, keepdims=True)
    srb[r] = jnp.broadcast_to(part_sum, (1, 128))
    across_rows(srb, sr_ss, sr_rs)
    total = sum(srb[k] for k in range(R))[:, 0:1]
    rms = jnp.sqrt(total / (C * Db * R * Fb))
    end_ref[0] = jnp.max(jnp.maximum(1.0, rms / CLIP_LEVEL))
    sent(stb.at[pl.ds(0, devices - 1)], st_ss)
    arrived(stb.at[pl.ds(0, devices - 1)], st_rs)
    lane = lax.broadcasted_iota(jnp.int32, (1, 128), 1)
    totals = jnp.sum(stb[...], axis=0)
    end_ref[1] = jnp.sum(jnp.where(lane == 1, totals, 0.0)) / batch
    for wait in finish:
        wait()


def divide(raw_ref, row_ref, col_ref, end_ref, upd_ref, nr_ref, nc_ref, loss_ref):
    upd_ref[...] = raw_ref[...] / end_ref[0]
    nr_ref[...] = row_ref[...]
    nc_ref[...] = col_ref[...]
    loss_ref[0] = end_ref[1]


def per_device(pooled, hidden, text, weight, row_moment, col_moment, log_scale, bias):
    R, C = lax.axis_size("row"), lax.axis_size("col")
    L, X, Z = LOW, R // CORES, C // LOW
    T, D = pooled.shape
    Db, Fb = weight.shape
    Dp = -(-Db // 16) * 16
    F2 = Z * Dp
    plane = R * L
    texts = X * C * T

    K = 3 if Dp % 48 == 0 else 1
    E = 1 if Z >= 4 else 0
    F2p = -(-F2 // 128) * 128
    Fw = max(-(-Dp // 128) * 128, F2p - (F2 - Dp) // 128 * 128)
    sizes = (R, C, X, Z, T, Db, Dp, Fb, K, E, F2, F2p, Fw)
    vmem = pl.BlockSpec(memory_space=pltpu.VMEM)
    smem = pl.BlockSpec(memory_space=pltpu.SMEM)
    dma = lambda *s: pltpu.SemaphoreType.DMA(s)
    one = pltpu.SemaphoreType.DMA
    raw = pl.pallas_call(
        functools.partial(kernel, sizes),
        out_shape=(
            jax.ShapeDtypeStruct((Db, Fb), F32),
            jax.ShapeDtypeStruct((Db,), F32),
            jax.ShapeDtypeStruct((Fb,), F32),
            jax.ShapeDtypeStruct((2,), F32),
        ),
        in_specs=[pl.BlockSpec(memory_space=pl.ANY)] * 6 + [smem] * 2,
        out_specs=(pl.BlockSpec(memory_space=pl.ANY),) * 3 + (smem,),
        scratch_shapes=[
            pltpu.VMEM((T, R * Fb), BF16),
            pltpu.VMEM((Db, Fb), F32),
            pltpu.VMEM((T, D), BF16),
            pltpu.VMEM((T, D), BF16),
            pltpu.VMEM((Db,), F32),
            pltpu.VMEM((Fb,), F32),
            pltpu.VMEM((R, T, Fb), BF16),
            pltpu.VMEM((T, L * F2), F32),
            pltpu.VMEM((Db, 1), F32),
            pltpu.VMEM((plane * T, Fb), BF16),
            pltpu.VMEM((F2p, Fb), BF16),
            pltpu.VMEM((texts, L * F2), BF16),
            pltpu.VMEM((plane * T, F2p), F32),
            pltpu.VMEM((X, L * T, F2p), F32),
            pltpu.VMEM((X, L * T, F2p), F32),
            pltpu.VMEM((X, L, T, F2p), F32),
            pltpu.VMEM((T, L * F2), F32),
            pltpu.VMEM((2 * T, L * F2), BF16),
            pltpu.VMEM((T, L * F2), F32),
            pltpu.VMEM((T, L * F2), F32),
            pltpu.VMEM((L, T, F2), BF16),
            pltpu.VMEM((plane * T, F2), BF16),
            pltpu.VMEM((F2, plane * T), BF16),
            pltpu.VMEM((Z, Dp, Fb), F32),
            pltpu.VMEM((Z, Dp, Fb), BF16),
            pltpu.VMEM((2, Z, Dp, Fb), BF16),
            pltpu.VMEM((Db, Fb), F32),
            pltpu.VMEM((Db,), F32),
            pltpu.VMEM((Fb,), F32),
            pltpu.VMEM((R, 1, Db), F32),
            pltpu.VMEM((C, 1, Fb), F32),
            pltpu.VMEM((R * C, 1, 128), F32),
            pltpu.VMEM((C, 1, Fb), F32),
            pltpu.VMEM((R, 1, 128), F32),
            pltpu.VMEM((plane * T, Fb), BF16),
            pltpu.VMEM((L, T, Dp), BF16),
            pltpu.VMEM((plane * T, Dp), BF16),
            dma(9),
            one, one, one, dma(2, Z), dma(Z), dma(2, Z), one, dma(X * C), one, one,
            one, dma(X, 2), one, dma(2), dma(2), dma(2),
            one, dma(plane), one, dma(2, Z, K), one, one, one, one, one, one,
            one, one, one, one, one, one, one, dma(plane),
        ],
        compiler_params=pltpu.CompilerParams(
            has_side_effects=True, collective_id=0, vmem_limit_bytes=60 * 1024 * 1024
        ),
    )(
        hidden, weight, pooled, text, row_moment, col_moment, log_scale[None], bias[None],
    )
    upd, nr, nc, loss = pl.pallas_call(
        divide,
        out_shape=(
            jax.ShapeDtypeStruct((Db, Fb), F32),
            jax.ShapeDtypeStruct((Db,), F32),
            jax.ShapeDtypeStruct((Fb,), F32),
            jax.ShapeDtypeStruct((1,), F32),
        ),
        in_specs=[vmem] * 3 + [smem],
        out_specs=(vmem,) * 3 + (smem,),
    )(*raw)
    return upd, nr, nc, loss[0]


def solution(mesh):
    return jax.shard_map(
        per_device,
        mesh=mesh,
        in_specs=(
            P(("row", "col"), None),
            P(("row", "col"), None),
            P(("row", "col"), None),
            P("col", "row"),
            P("col"),
            P("row"),
            P(),
            P(),
        ),
        out_specs=(P("col", "row"), P("col"), P("row"), P()),
        check_vma=False,
    )
```

```python
import functools

import jax
import jax.numpy as jnp
from jax import lax
from jax.experimental import pallas as pl
from jax.experimental.pallas import tpu as pltpu
from jax.sharding import PartitionSpec as P

EPSILON = 1e-06
DECAY_RATE = 0.8
CLIP_LEVEL = 1.0
FLOOR_VALUE = 1e-30
CORES = 2
LOW = 2
MESH = pl.DeviceIdType.MESH
F32 = jnp.float32
BF16 = jnp.bfloat16


def dot_nt(a, b):
    return lax.dot_general(a, b, (((1,), (1,)), ((), ())), preferred_element_type=F32)


def kernel(
    sizes,
    hid_in, w_in, pool_in, text_in, rm_in, cm_in, ls_ref, bias_ref,
    upd_out, nr_out, nc_out, end_ref,
    hv, wv, pv, tv, rmv, cmv, hs, pool, rmc,
    hid, wg, txa, part, pre, summed, proj, mix, imgs, ug_s, ug_r, mg_s, mga, turned, gp, gz_s, gz,
    upd_ref, nr_ref, nc_ref, end_v, rsb, csb, qcb, srb, hid2, mgx_s, mgx, ld,
    hid_ss, hid_rs, hx_rs, w_ss, w_rs, tz_ss, tp_ss, t_rs, td_ss, td_rs, pp_ss, pp_rs, p_ss, p_rs, pair_ss, pair_rs,
    mg_ss, mg_rs, g_ss, g_rs, row_ss, row_rs, col_ss, col_rs,
    qc_ss, qc_rs, sr_ss, sr_rs, hf_ss, hf_rs, mgx_ss, mgx_rs,
):
    R, C, X, Z, T, Db, Dp, Fb, K, E, F2, F2p, Fw = sizes
    L = LOW
    plane = R * L
    devices = R * C
    batch = devices * T
    r = lax.axis_index("row")
    c = lax.axis_index("col")
    z, y = c // L, c % L
    x, core = r // CORES, r % CORES
    q = r * L + y
    finish = []
    Dc = Dp // K

    loads = [
        pltpu.make_async_copy(src, dst, ld.at[i])
        for i, (src, dst) in enumerate(
            ((w_in, wv), (hid_in, hv), (text_in, tv), (pool_in, pv), (rm_in, rmv), (cm_in, cmv))
        )
    ]
    for load in loads:
        load.start()
    barrier = pltpu.get_barrier_semaphore()

    def greet(device):
        pl.semaphore_signal(barrier, inc=1, device_id=device, device_id_type=MESH)

    for o in range(1, plane):
        other = lax.rem(q + o, plane)
        greet((other // L, z * L + other % L))
    pl.when(z > 0)(lambda: greet((r, c - L)))
    pl.when(z < Z - 1)(lambda: greet((r, c + L)))

    def send(src, dst, ss, rs, device, cond=None, bulk=False):
        def make():
            return pltpu.make_async_remote_copy(
                src_ref=src, dst_ref=dst, send_sem=ss, recv_sem=rs,
                device_id=device, device_id_type=MESH,
            )

        if cond is None:
            make().start()
        else:
            pl.when(cond)(lambda: make().start())
        if bulk:
            return
        if cond is None:
            finish.append(lambda: make().wait_send())
        else:
            finish.append(lambda: pl.when(cond)(lambda: make().wait_send()))

    def sent(like, ss):
        finish.append(lambda: pltpu.make_async_copy(like, like, ss).wait())

    def arrived(slot, rs):
        pltpu.make_async_copy(slot, slot, rs).wait()

    def rows(index, count):
        return pl.ds(pl.multiple_of(index * count, count), count)

    def by_half(value, store):
        for h in range(L):
            for k in range(Z):
                at = (k * L + h) * Db
                store(h * F2 + k * Dp, value[:, at:at + Db])

    own_slot = (z * X + x) * L + y
    loads[0].wait()
    if Dp != Db:
        wg[rows(z, Dp)] = jnp.zeros((Dp, Fb), BF16)
        txa[rows(own_slot, T)] = jnp.zeros((T, L * F2), BF16)
        pool[...] = jnp.zeros(pool.shape, F32)
    wg[pl.ds(pl.multiple_of(z * Dp, Dp), Db)] = wv[...].astype(BF16)
    if F2p != F2:
        wg[F2:F2p] = jnp.zeros((F2p - F2, Fb), BF16)
    loads[1].wait()
    for k in range(R):
        hs[k] = hv[:, k * Fb:(k + 1) * Fb]
    hid[rows(q, T)] = hs[r]
    loads[2].wait()
    tf = tv[...].astype(F32)
    tn = tf / jnp.sqrt(jnp.sum(tf * tf, axis=1, keepdims=True) + EPSILON)

    def put_text(at, value):
        txa[rows(own_slot, T), at:at + Db] = value.astype(BF16)

    by_half(tn, put_text)
    pl.semaphore_wait(barrier, plane - 1 + jnp.where(z > 0, 1, 0) + jnp.where(z < Z - 1, 1, 0))
    across = [lax.rem(x + o, X) for o in range(1, X)]
    beside = [lax.rem(y + o, L) for o in range(1, L)]
    partner = (x * CORES + (1 - core), c)
    own_rows = hid.at[rows(q, T)]
    for x2 in across:
        for k in range(CORES):
            r2 = x2 * CORES + k
            send(hs.at[r2], own_rows, hid_ss, hx_rs, (r2, c), bulk=True)
    for y2 in beside:
        for k in range(CORES):
            r2 = x * CORES + k
            send(hs.at[r2], own_rows, hid_ss, hid_rs, (r2, z * L + y2), bulk=True)
    send(hs.at[partner[0]], own_rows, hid_ss, hid_rs, partner, bulk=True)
    crossing = (X - 1) * CORES
    relayed = crossing * (L - 1)
    direct = crossing + CORES * (L - 1) + 1

    def hidden_on():
        arrived(hid.at[pl.ds(0, crossing * T)], hx_rs)
        for x2 in across:
            for k in range(CORES):
                at = hid.at[rows((x2 * CORES + k) * L + y, T)]
                for y2 in beside:
                    send(at, at, hid_ss, hid_rs, (r, z * L + y2), bulk=True)
        sent(hid.at[pl.ds(0, (direct + relayed) * T)], hid_ss)

    def text_place(zs):
        return (zs * X + x) * L + y

    def neighbours():
        along_x = [(lax.rem(x + o, X), y) for o in range(1, X)]
        return along_x + [(x, lax.rem(y + o, L)) for o in range(1, L)]

    low = z < Z // 2
    final = jnp.where(low, Z - 1, 0)
    edge = jnp.logical_and(E > 0, jnp.logical_or(z == 0, z == Z - 1))
    nearby = jnp.logical_and(E > 0, jnp.logical_or(z == 1, z == Z - 2))
    nest = jnp.where(low, 1, Z - 2)

    def relay(s):
        split = T // 4 if s < 2 else T // 2
        for d, direction in enumerate((1, -1)):
            if s == 0 and d:
                continue
            zs = z - direction * s
            has = jnp.logical_and(zs >= 0, zs < Z)
            block = jnp.clip(zs, 0, Z - 1)
            for n, (x2, y2) in enumerate(neighbours()):
                place = (block * X + x2) * L + y2
                at = txa.at[rows(place, T)]
                if s:
                    pl.when(has)(lambda: arrived(at, t_rs.at[place]))
                else:
                    arrived(at, t_rs.at[place])
                h = 0 if n < X - 1 else 1
                part_at = pl.multiple_of(place * T + h * split, split)
                half = txa.at[pl.ds(part_at, T - split if h else split)]
                onward = neighbours()[X - 1:] if h == 0 else neighbours()[:X - 1]
                for x3, y3 in onward:
                    send(
                        half, half, td_ss, td_rs,
                        (x3 * CORES + core, z * L + y3), has if s else None, True,
                    )

    def texts_on(s):
        for d, direction in enumerate((1, -1)):
            zs = z - direction * s
            nz = z + direction
            has = jnp.logical_and(zs >= 0, zs < Z)
            go = jnp.logical_and(has, jnp.logical_and(nz >= 0, nz < Z))
            place = text_place(jnp.clip(zs, 0, Z - 1))
            at = txa.at[rows(place, T)]
            if s:
                pl.when(has)(lambda: arrived(at, t_rs.at[place]))
            send(at, at, tz_ss.at[d, s], t_rs.at[place], (r, jnp.clip(nz, 0, Z - 1) * L + y), go)
            if s or d == 0:
                for x2, y2 in neighbours():
                    send(
                        at, at, tp_ss, t_rs.at[place],
                        (x2 * CORES + core, z * L + y2), has if s else None, True,
                    )

    def weights_on(s):
        for d, direction in enumerate((1, -1)):
            zs = z - direction * s
            nz = z + direction
            has = jnp.logical_and(zs >= 0, zs < Z)
            go = jnp.logical_and(has, jnp.logical_and(nz >= 0, nz < Z))
            block = jnp.clip(zs, 0, Z - 1)
            at = wg.at[rows(block, Dp)]
            if s:
                pl.when(has)(lambda: arrived(at, w_rs.at[block]))
            send(at, at, w_ss.at[d, s], w_rs.at[block], (r, jnp.clip(nz, 0, Z - 1) * L + y), go)

    texts_on(0)
    weights_on(0)
    loads[3].wait()

    def put_pool(at, value):
        pool[:, at:at + Db] = value

    by_half(pv[...].astype(F32), put_pool)
    loads[4].wait()
    loads[5].wait()
    eye = lax.broadcasted_iota(jnp.int32, (Db, Db), 0) == lax.broadcasted_iota(jnp.int32, (Db, Db), 1)
    line = jnp.broadcast_to(rmv[...].reshape(1, Db), (Db, Db))
    rmc[...] = jnp.sum(jnp.where(eye, line, 0.0), axis=1, keepdims=True)
    spans = (
        (pl.multiple_of(jnp.where(low, 0, Fw), 128), F2p - Fw),
        (pl.multiple_of(jnp.where(low, F2p - Fw, 0), 128), Fw),
    )

    def project(g):
        start, width = spans[g]
        lanes = pl.ds(start, width)
        for side in (1 - core, core):
            for o in range(1, X + 1):
                x2 = lax.rem(x + o, X)
                at = rows(x2 * CORES + side, L * T)
                part[at, lanes] = dot_nt(hid[at], wg[lanes])
                if side is not core:
                    send(part.at[at, lanes], pre.at[x2, :, lanes], pp_ss, pp_rs.at[x2, g], partner, bulk=True)

    def spread(g):
        start, width = spans[g]
        lanes = pl.ds(start, width)
        for o in range(1, X + 1):
            x2 = lax.rem(x + o, X)
            arrived(pre.at[x2, :, lanes], pp_rs.at[x2, g])
            summed[x2, :, lanes] = part[rows(x2 * CORES + core, L * T), lanes] + pre[x2, :, lanes]
            for k in range(L):
                y2 = lax.rem(y + 1 + k, L)
                if o == X and k == L - 1:
                    proj[x, y, :, lanes] = summed[x, rows(y, T), lanes]
                else:
                    send(
                        summed.at[x2, rows(y2, T), lanes], proj.at[x, y, :, lanes], p_ss,
                        p_rs.at[g], (x2 * CORES + core, z * L + y2), bulk=True,
                    )

    def gathered(g):
        start, width = spans[g]
        arrived(part.at[pl.ds(0, (X * L - 1) * T), pl.ds(start, width)], p_rs.at[g])

    for s in range(1, Z):
        texts_on(s)
        if s == 1:
            hidden_on()
        if s == Z - 1:
            spread(0)
        else:
            weights_on(s)
        relay(s - 1)
        if s == Z - 2:
            arrived(hid.at[pl.ds(0, (plane - 1 - crossing) * T)], hid_rs)
            if E:
                send(hid, hid2, hf_ss, hf_rs, (r, nest * L + y), edge)
            project(0)
    weights_on(Z - 1)
    project(1)
    sent(part.at[pl.ds(0, X * L * T)], pp_ss)
    sent(part.at[pl.ds(0, (X * L - 1) * T)], p_ss)
    relay(Z - 1)
    spread(1)
    pairs_each = (X - 1) * (L - 1) * T
    sent(txa.at[pl.ds(0, Z * pairs_each)], td_ss)
    sent(txa.at[pl.ds(0, Z * (X + L - 2) * T)], tp_ss)
    gathered(0)
    gathered(1)
    for h in range(L):
        total = proj[0, h]
        for k in range(1, X):
            total = total + proj[k, h]
        mix[:, h * F2:(h + 1) * F2] = total[:, :F2]
    mixed = mix[...] + pool[...]
    length = jnp.sqrt(jnp.sum(mixed * mixed, axis=1, keepdims=True) + EPSILON)
    unit = mixed / length
    imgs[:T] = unit.astype(BF16)
    theirs = imgs.at[pl.ds(T, T)]
    send(imgs.at[pl.ds(0, T)], theirs, pair_ss.at[0], pair_rs.at[0], partner)
    scale = jnp.exp(jnp.full((1, 1), ls_ref[0], F32))
    bias = jnp.full((1, 1), bias_ref[0], F32)
    width = X * L * T

    def pairs(top, count, zs, blocks=1):
        images = imgs[top:top + count]
        texts = txa[pl.ds(pl.multiple_of(zs * width, width), blocks * width)]
        logits = scale * dot_nt(images, texts) + bias
        row_id = lax.broadcasted_iota(jnp.int32, logits.shape, 0) + top
        col_id = lax.broadcasted_iota(jnp.int32, logits.shape, 1) + (zs * width - own_slot * T)
        match = jnp.logical_and(row_id == col_id, row_id < T)
        u = jnp.where(match, -logits, logits)
        e = jnp.exp(-jnp.abs(u))
        loss = jnp.sum(jnp.maximum(u, 0.0) + jnp.log1p(e), axis=1, keepdims=True)
        sig = jnp.where(u >= 0, F32(1.0), e) / (1.0 + e)
        pg = (jnp.where(match, -sig, sig) / batch).astype(BF16)
        return loss, jnp.dot(pg, texts, preferred_element_type=F32)

    def total(top):
        loss, grads = pairs(top, T, 0, wide)
        if Z <= wide:
            return loss, grads

        def more(k, carry):
            loss, grads = pairs(top, T, k * wide, wide)
            return carry[0] + loss, carry[1] + grads

        return lax.fori_loop(1, Z // wide, more, (loss, grads))

    wide = max(w for w in (1, 2, 4) if Z % w == 0)
    arrived(txa.at[pl.ds(0, Z * pairs_each)], td_rs)
    loss_a, grads_a = total(0)
    arrived(theirs, pair_rs.at[0])
    loss_b, grads_b = total(T)
    ug_s[...] = scale * grads_b
    send(ug_s, ug_r, pair_ss.at[1], pair_rs.at[1], partner)
    arrived(ug_r, pair_rs.at[1])
    ug = scale * grads_a + ug_r[...]
    inner = jnp.sum(unit * ug, axis=1, keepdims=True)
    mg = ((ug - unit * inner) / length).astype(BF16)
    for h in range(L):
        mg_s[h] = mg[:, h * F2:(h + 1) * F2]
    others = [
        (lax.rem(x + ox, X), lax.rem(y + oy, L))
        for ox in reversed(range(X)) for oy in reversed(range(L)) if ox or oy
    ]
    everyone = others + [(x, y)]
    if E:
        for h in range(L):
            top = mg[:, h * F2 + (Z - 1) * Dp:h * F2 + Z * Dp]
            mgx_s[h] = jnp.where(low, top, mg[:, h * F2:h * F2 + Dp])
        for x2, y2 in everyone:
            send(
                mgx_s.at[y2], mgx.at[rows(q, T)], mgx_ss, mgx_rs.at[q],
                (x2 * CORES + core, nest * L + y2), edge, True,
            )
    for x2, y2 in others:
        send(
            mg_s.at[y2], mga.at[rows(q, T)], mg_ss, mg_rs.at[q],
            (x2 * CORES + core, z * L + y2), bulk=True,
        )
    send(mg_s.at[y], mga.at[rows(q, T)], mg_ss, mg_rs.at[q], partner, bulk=True)
    mga[rows(q, T)] = mg_s[y]
    loss_local = jnp.sum(loss_a + loss_b, axis=0, keepdims=True)
    csb[c, :, Fb:Fb + 1] = loss_local
    for x2, y2 in others:
        source = (x2 * CORES + core) * L + y2
        at = mga.at[rows(source, T)]
        arrived(at, mg_rs.at[source])
        send(at, at, mg_ss, mg_rs.at[source], partner, bulk=True)
    sent(mga.at[pl.ds(0, (plane - 1) * T)], mg_ss)
    if E:
        finish.append(lambda: pl.when(jnp.logical_or(edge, nearby))(
            lambda: arrived(mgx.at[pl.ds(0, X * L * T)], mgx_ss)
        ))
    for x2, y2 in [(x, y)] + others:
        source = (x2 * CORES + 1 - core) * L + y2
        arrived(mga.at[rows(source, T)], mg_rs.at[source])

    turned[...] = mga[...].T

    def own_part(zd):
        gp[zd] = jnp.dot(turned[rows(zd, Dp)], hid[...], preferred_element_type=F32)

    def far_part():
        for x2, y2 in everyone:
            at = mgx.at[rows((x2 * CORES + core) * L + y2, T)]
            arrived(at, mgx_rs.at[(x2 * CORES + core) * L + y2])
            send(at, at, mgx_ss, mgx_rs.at[(x2 * CORES + core) * L + y2], partner, bulk=True)
        arrived(hid2, hf_rs)
        for x2, y2 in everyone:
            source = (x2 * CORES + 1 - core) * L + y2
            arrived(mgx.at[rows(source, T)], mgx_rs.at[source])
        gp[final] = gp[final] + jnp.dot(mgx[...].T, hid2[...], preferred_element_type=F32)

    def pieces(tau, d):
        place = z if d == 0 else Z - 1 - z
        far = Z - 1 if d == 0 else 0
        i = tau - 2 * jnp.maximum(place - E, 0) + jnp.where(place == 0, K * E, 0)
        zd = jnp.clip(i, 0, Z * K - 1) // K
        k = jnp.clip(i, 0, Z * K - 1) % K
        zd = Z - 1 - zd if d == 0 else zd
        beyond = zd > z if d == 0 else zd < z
        ready = jnp.logical_and(i >= 0, i < Z * K)
        opens = jnp.logical_or(place == 0, jnp.logical_and(place == E, zd == far))
        return zd, k, jnp.logical_and(ready, beyond), jnp.logical_and(ready, zd == z), opens, place

    def step(tau, held):
        for d in range(2):
            zd, k, passing, ending, opens, place = pieces(tau, d)
            cut = rows(k, Dc)
            at = gz.at[d, zd, cut]
            copy = pltpu.make_async_remote_copy(
                src_ref=gz_s.at[zd, cut], dst_ref=at, send_sem=g_ss, recv_sem=g_rs.at[zd + 1 - d, k],
                device_id=(r, jnp.clip(z + (1 if d == 0 else -1), 0, Z - 1) * L + y), device_id_type=MESH,
            )

            def first():
                gz_s[zd, cut] = gp[zd, cut].astype(BF16)
                copy.start()

            def onward():
                arrived(at, g_rs.at[zd + 1 - d, k])
                gz_s[zd, cut] = (gp[zd, cut] + at[...].astype(F32)).astype(BF16)
                copy.start()

            def last():
                arrived(at, g_rs.at[zd + 1 - d, k])
                gp[zd, cut] = gp[zd, cut] + at[...].astype(F32)

            passing = jnp.logical_and(passing, held)
            ending = jnp.logical_and(jnp.logical_and(ending, held), place > 0)
            pl.when(jnp.logical_and(passing, opens))(first)
            pl.when(jnp.logical_and(passing, jnp.logical_not(opens)))(onward)
            pl.when(ending)(last)

    def early(tau, _):
        step(tau, edge)
        return _

    def later(tau, _):
        step(tau, jnp.logical_or(jnp.logical_not(edge), tau >= head))
        return _

    steps_g = max((Z - 1) * K + 1 - 2 * E, K - 1 + 2 * (Z - 1 - E)) + 1
    head = min(K, 2)

    def order(k):
        return jnp.where(low, Z - 1 - k, k)

    if E:
        own_part(order(1))
        lax.fori_loop(0, head, early, 0)
        pl.when(jnp.logical_not(edge))(lambda: own_part(order(0)))
        for k in range(2, Z):
            own_part(order(k))
        pl.when(nearby)(far_part)
        finish.append(lambda: pl.when(edge)(lambda: arrived(gz_s.at[pl.ds(0, Z - 2)], g_ss)))
        finish.append(lambda: pl.when(jnp.logical_not(edge))(lambda: arrived(gz_s.at[pl.ds(0, Z - 1)], g_ss)))
    else:
        for k in range(Z):
            own_part(order(k))
        sent(gz_s.at[pl.ds(0, Z - 1)], g_ss)
    lax.fori_loop(0, steps_g, later, 0)
    g = gp[z][:Db]

    def across_cols(box, ss, rs):
        for o in range(1, C):
            send(box.at[c], box.at[c], ss, rs, (r, lax.rem(c + o, C)), bulk=True)
        sent(box.at[pl.ds(0, C - 1)], ss)

    def across_rows(box, ss, rs, also=lambda: None):
        for o in range(1, R):
            send(box.at[r], box.at[r], ss, rs, (lax.rem(r + o, R), c), bulk=True)
        sent(box.at[pl.ds(0, R - 1)], ss)
        also()
        arrived(box.at[pl.ds(0, R - 1)], rs)

    square = g * g
    sq = square + FLOOR_VALUE
    rsb[r] = jnp.sum(jnp.where(eye, jnp.sum(sq, axis=1, keepdims=True), 0.0), axis=0, keepdims=True)
    csb[c, :, :Fb] = jnp.sum(sq, axis=0, keepdims=True)
    across_rows(rsb, row_ss, row_rs, lambda: across_cols(csb, col_ss, col_rs))
    row_sum = jnp.broadcast_to(sum(rsb[k] for k in range(R)), (Db, Db))
    row_sum = jnp.sum(jnp.where(eye, row_sum, 0.0), axis=1, keepdims=True)
    new_row = DECAY_RATE * rmc[...] + (1.0 - DECAY_RATE) * row_sum / (R * Fb)
    qcb[c] = jnp.sum(square / new_row, axis=0, keepdims=True)
    across_cols(qcb, qc_ss, qc_rs)
    nr_ref[...] = jnp.sum(jnp.where(eye, new_row, 0.0), axis=0)
    arrived(csb.at[pl.ds(0, C - 1)], col_rs)
    col_sum = sum(csb[k] for k in range(C))
    new_col = DECAY_RATE * cmv[...].reshape(1, Fb) + (1.0 - DECAY_RATE) * col_sum[:, :Fb] / (C * Db)
    nc_ref[...] = new_col[0]
    upd_ref[...] = g / jnp.sqrt(new_row * new_col)
    for i, (src, dst) in enumerate(((upd_ref, upd_out), (nr_ref, nr_out), (nc_ref, nc_out))):
        store = pltpu.make_async_copy(src, dst, ld.at[6 + i])
        store.start()
        finish.append(store.wait)
    arrived(qcb.at[pl.ds(0, C - 1)], qc_rs)
    part_sum = jnp.sum(sum(qcb[k] for k in range(C)) / new_col, axis=1, keepdims=True)
    lane = lax.broadcasted_iota(jnp.int32, (1, 128), 1)
    srb[r] = jnp.where(lane == 0, part_sum, col_sum[:, Fb:Fb + 1])
    across_rows(srb, sr_ss, sr_rs)
    totals = sum(srb[k] for k in range(R))
    rms = jnp.sqrt(totals / (C * Db * R * Fb))
    end_v[...] = jnp.where(lane == 0, jnp.maximum(1.0, rms / CLIP_LEVEL), totals / batch)
    store = pltpu.make_async_copy(end_v, end_ref, ld.at[9])
    store.start()
    finish.append(store.wait)
    for wait in finish:
        wait()


def divide(raw_ref, row_ref, col_ref, end_ref, upd_ref, nr_ref, nc_ref, loss_ref):
    upd_ref[...] = raw_ref[...] / end_ref[:, 0:1]
    nr_ref[...] = row_ref[...]
    nc_ref[...] = col_ref[...]
    lane = lax.broadcasted_iota(jnp.int32, (1, 128), 1)
    loss_ref[0] = jnp.sum(jnp.where(lane == 1, end_ref[...], 0.0))


def per_device(pooled, hidden, text, weight, row_moment, col_moment, log_scale, bias):
    R, C = lax.axis_size("row"), lax.axis_size("col")
    L, X, Z = LOW, R // CORES, C // LOW
    T, D = pooled.shape
    Db, Fb = weight.shape
    Dp = -(-Db // 16) * 16
    F2 = Z * Dp
    plane = R * L
    texts = X * C * T

    K = 3 if Dp % 48 == 0 else 1
    E = 1 if Z >= 4 else 0
    F2p = -(-F2 // 128) * 128
    Fw = max(-(-Dp // 128) * 128, F2p - (F2 - Dp) // 128 * 128)
    sizes = (R, C, X, Z, T, Db, Dp, Fb, K, E, F2, F2p, Fw)
    vmem = pl.BlockSpec(memory_space=pltpu.VMEM)
    smem = pl.BlockSpec(memory_space=pltpu.SMEM)
    dma = lambda *s: pltpu.SemaphoreType.DMA(s)
    one = pltpu.SemaphoreType.DMA
    raw = pl.pallas_call(
        functools.partial(kernel, sizes),
        out_shape=(
            jax.ShapeDtypeStruct((Db, Fb), F32),
            jax.ShapeDtypeStruct((Db,), F32),
            jax.ShapeDtypeStruct((Fb,), F32),
            jax.ShapeDtypeStruct((1, 128), F32),
        ),
        in_specs=[pl.BlockSpec(memory_space=pl.ANY)] * 6 + [smem] * 2,
        out_specs=(pl.BlockSpec(memory_space=pl.ANY),) * 4,
        scratch_shapes=[
            pltpu.VMEM((T, R * Fb), BF16),
            pltpu.VMEM((Db, Fb), F32),
            pltpu.VMEM((T, D), BF16),
            pltpu.VMEM((T, D), BF16),
            pltpu.VMEM((Db,), F32),
            pltpu.VMEM((Fb,), F32),
            pltpu.VMEM((R, T, Fb), BF16),
            pltpu.VMEM((T, L * F2), F32),
            pltpu.VMEM((Db, 1), F32),
            pltpu.VMEM((plane * T, Fb), BF16),
            pltpu.VMEM((F2p, Fb), BF16),
            pltpu.VMEM((texts, L * F2), BF16),
            pltpu.VMEM((plane * T, F2p), F32),
            pltpu.VMEM((X, L * T, F2p), F32),
            pltpu.VMEM((X, L * T, F2p), F32),
            pltpu.VMEM((X, L, T, F2p), F32),
            pltpu.VMEM((T, L * F2), F32),
            pltpu.VMEM((2 * T, L * F2), BF16),
            pltpu.VMEM((T, L * F2), F32),
            pltpu.VMEM((T, L * F2), F32),
            pltpu.VMEM((L, T, F2), BF16),
            pltpu.VMEM((plane * T, F2), BF16),
            pltpu.VMEM((F2, plane * T), BF16),
            pltpu.VMEM((Z, Dp, Fb), F32),
            pltpu.VMEM((Z, Dp, Fb), BF16),
            pltpu.VMEM((2, Z, Dp, Fb), BF16),
            pltpu.VMEM((Db, Fb), F32),
            pltpu.VMEM((Db,), F32),
            pltpu.VMEM((Fb,), F32),
            pltpu.VMEM((1, 128), F32),
            pltpu.VMEM((R, 1, Db), F32),
            pltpu.VMEM((C, 1, Fb + 1), F32),
            pltpu.VMEM((C, 1, Fb), F32),
            pltpu.VMEM((R, 1, 128), F32),
            pltpu.VMEM((plane * T, Fb), BF16),
            pltpu.VMEM((L, T, Dp), BF16),
            pltpu.VMEM((plane * T, Dp), BF16),
            dma(10),
            one, one, one, dma(2, Z), dma(Z), dma(2, Z), one, dma(X * C), one, one,
            one, dma(X, 2), one, dma(2), dma(2), dma(2),
            one, dma(plane), one, dma(Z + 1, K), one, one, one, one,
            one, one, one, one, one, one, one, dma(plane),
        ],
        compiler_params=pltpu.CompilerParams(
            has_side_effects=True, collective_id=0, vmem_limit_bytes=60 * 1024 * 1024
        ),
    )(
        hidden, weight, pooled, text, row_moment, col_moment, log_scale[None], bias[None],
    )
    upd, nr, nc, loss = pl.pallas_call(
        divide,
        out_shape=(
            jax.ShapeDtypeStruct((Db, Fb), F32),
            jax.ShapeDtypeStruct((Db,), F32),
            jax.ShapeDtypeStruct((Fb,), F32),
            jax.ShapeDtypeStruct((1,), F32),
        ),
        in_specs=[vmem] * 4,
        out_specs=(vmem,) * 3 + (smem,),
    )(*raw)
    return upd, nr, nc, loss[0]


def solution(mesh):
    return jax.shard_map(
        per_device,
        mesh=mesh,
        in_specs=(
            P(("row", "col"), None),
            P(("row", "col"), None),
            P(("row", "col"), None),
            P("col", "row"),
            P("col"),
            P("row"),
            P(),
            P(),
        ),
        out_specs=(P("col", "row"), P("col"), P("row"), P()),
        check_vma=False,
    )
```

```python
import functools

import jax
import jax.numpy as jnp
from jax import lax
from jax.experimental import pallas as pl
from jax.experimental.pallas import tpu as pltpu
from jax.sharding import PartitionSpec as P

EPSILON = 1e-06
DECAY_RATE = 0.8
CLIP_LEVEL = 1.0
FLOOR_VALUE = 1e-30
CORES = 2
LOW = 2
MESH = pl.DeviceIdType.MESH
F32 = jnp.float32
BF16 = jnp.bfloat16


def dot_nt(a, b):
    return lax.dot_general(a, b, (((1,), (1,)), ((), ())), preferred_element_type=F32)


def kernel(
    sizes,
    hid_in, w_in, pool_in, text_in, rm_in, cm_in, ls_ref, bias_ref,
    upd_out, nr_out, nc_out, end_ref,
    hv, wv, pv, tv, rmv, cmv, hs, pool, rmc,
    hid, wg, txa, part, pre, summed, proj, mix, imgs, ug_s, ug_r, mg_s, mga, turned, gp, gz_s, gz,
    upd_ref, nr_ref, nc_ref, end_v, rsb, csb, qcb, srb, hid2, mgx_s, mgx, ld,
    hid_ss, hid_rs, hx_rs, w_ss, w_rs, tz_ss, tp_ss, t_rs, td_ss, td_rs, pp_ss, pp_rs, p_ss, p_rs, pair_ss, pair_rs,
    mg_ss, mg_rs, g_ss, g_rs, row_ss, row_rs, col_ss, col_rs,
    qc_ss, qc_rs, sr_ss, sr_rs, hf_ss, hf_rs, mgx_ss, mgx_rs,
):
    R, C, X, Z, T, Db, Dp, Fb, K, E, F2, F2p, Fw = sizes
    L = LOW
    plane = R * L
    devices = R * C
    batch = devices * T
    r = lax.axis_index("row")
    c = lax.axis_index("col")
    z, y = c // L, c % L
    x, core = r // CORES, r % CORES
    q = r * L + y
    finish = []
    Dc = Dp // K

    loads = [
        pltpu.make_async_copy(src, dst, ld.at[i])
        for i, (src, dst) in enumerate(
            ((w_in, wv), (hid_in, hv), (text_in, tv), (pool_in, pv), (rm_in, rmv), (cm_in, cmv))
        )
    ]
    for load in loads:
        load.start()
    barrier = pltpu.get_barrier_semaphore()

    def greet(device):
        pl.semaphore_signal(barrier, inc=1, device_id=device, device_id_type=MESH)

    for o in range(1, plane):
        other = lax.rem(q + o, plane)
        greet((other // L, z * L + other % L))
    pl.when(z > 0)(lambda: greet((r, c - L)))
    pl.when(z < Z - 1)(lambda: greet((r, c + L)))

    def send(src, dst, ss, rs, device, cond=None, bulk=False):
        def make():
            return pltpu.make_async_remote_copy(
                src_ref=src, dst_ref=dst, send_sem=ss, recv_sem=rs,
                device_id=device, device_id_type=MESH,
            )

        if cond is None:
            make().start()
        else:
            pl.when(cond)(lambda: make().start())
        if bulk:
            return
        if cond is None:
            finish.append(lambda: make().wait_send())
        else:
            finish.append(lambda: pl.when(cond)(lambda: make().wait_send()))

    def sent(like, ss):
        finish.append(lambda: pltpu.make_async_copy(like, like, ss).wait())

    def arrived(slot, rs):
        pltpu.make_async_copy(slot, slot, rs).wait()

    def rows(index, count):
        return pl.ds(pl.multiple_of(index * count, count), count)

    def by_half(value, store):
        for h in range(L):
            for k in range(Z):
                at = (k * L + h) * Db
                store(h * F2 + k * Dp, value[:, at:at + Db])

    own_slot = (z * X + x) * L + y
    loads[0].wait()
    if Dp != Db:
        wg[rows(z, Dp)] = jnp.zeros((Dp, Fb), BF16)
        txa[rows(own_slot, T)] = jnp.zeros((T, L * F2), BF16)
        pool[...] = jnp.zeros(pool.shape, F32)
    wg[pl.ds(pl.multiple_of(z * Dp, Dp), Db)] = wv[...].astype(BF16)
    if F2p != F2:
        wg[F2:F2p] = jnp.zeros((F2p - F2, Fb), BF16)
    loads[1].wait()
    for k in range(R):
        hs[k] = hv[:, k * Fb:(k + 1) * Fb]
    hid[rows(q, T)] = hs[r]
    loads[2].wait()
    tf = tv[...].astype(F32)
    tn = tf / jnp.sqrt(jnp.sum(tf * tf, axis=1, keepdims=True) + EPSILON)

    def put_text(at, value):
        txa[rows(own_slot, T), at:at + Db] = value.astype(BF16)

    by_half(tn, put_text)
    pl.semaphore_wait(barrier, plane - 1 + jnp.where(z > 0, 1, 0) + jnp.where(z < Z - 1, 1, 0))
    across = [lax.rem(x + o, X) for o in range(1, X)]
    beside = [lax.rem(y + o, L) for o in range(1, L)]
    partner = (x * CORES + (1 - core), c)
    own_rows = hid.at[rows(q, T)]
    for x2 in across:
        for k in range(CORES):
            r2 = x2 * CORES + k
            send(hs.at[r2], own_rows, hid_ss, hx_rs, (r2, c), bulk=True)
    for y2 in beside:
        for k in range(CORES):
            r2 = x * CORES + k
            send(hs.at[r2], own_rows, hid_ss, hid_rs, (r2, z * L + y2), bulk=True)
    send(hs.at[partner[0]], own_rows, hid_ss, hid_rs, partner, bulk=True)
    crossing = (X - 1) * CORES
    relayed = crossing * (L - 1)
    direct = crossing + CORES * (L - 1) + 1

    def hidden_on():
        arrived(hid.at[pl.ds(0, crossing * T)], hx_rs)
        for x2 in across:
            for k in range(CORES):
                at = hid.at[rows((x2 * CORES + k) * L + y, T)]
                for y2 in beside:
                    send(at, at, hid_ss, hid_rs, (r, z * L + y2), bulk=True)
        sent(hid.at[pl.ds(0, (direct + relayed) * T)], hid_ss)

    def text_place(zs):
        return (zs * X + x) * L + y

    def neighbours():
        along_x = [(lax.rem(x + o, X), y) for o in range(1, X)]
        return along_x + [(x, lax.rem(y + o, L)) for o in range(1, L)]

    low = z < Z // 2
    final = jnp.where(low, Z - 1, 0)
    edge = jnp.logical_and(E > 0, jnp.logical_or(z == 0, z == Z - 1))
    nearby = jnp.logical_and(E > 0, jnp.logical_or(z == 2, z == Z - 3))
    nest = jnp.where(low, 2, Z - 3)
    theirs_far = jnp.where(z == 2, Z - 1, 0)

    def relay(s):
        split = T // 4 if s < 2 else T // 2
        for d, direction in enumerate((1, -1)):
            if s == 0 and d:
                continue
            zs = z - direction * s
            has = jnp.logical_and(zs >= 0, zs < Z)
            block = jnp.clip(zs, 0, Z - 1)
            for n, (x2, y2) in enumerate(neighbours()):
                place = (block * X + x2) * L + y2
                at = txa.at[rows(place, T)]
                if s:
                    pl.when(has)(lambda: arrived(at, t_rs.at[place]))
                else:
                    arrived(at, t_rs.at[place])
                h = 0 if n < X - 1 else 1
                part_at = pl.multiple_of(place * T + h * split, split)
                half = txa.at[pl.ds(part_at, T - split if h else split)]
                onward = neighbours()[X - 1:] if h == 0 else neighbours()[:X - 1]
                for x3, y3 in onward:
                    send(
                        half, half, td_ss, td_rs,
                        (x3 * CORES + core, z * L + y3), has if s else None, True,
                    )

    def texts_on(s):
        for d, direction in enumerate((1, -1)):
            zs = z - direction * s
            nz = z + direction
            has = jnp.logical_and(zs >= 0, zs < Z)
            go = jnp.logical_and(has, jnp.logical_and(nz >= 0, nz < Z))
            place = text_place(jnp.clip(zs, 0, Z - 1))
            at = txa.at[rows(place, T)]
            if s:
                pl.when(has)(lambda: arrived(at, t_rs.at[place]))
            send(at, at, tz_ss.at[d, s], t_rs.at[place], (r, jnp.clip(nz, 0, Z - 1) * L + y), go)
            if s or d == 0:
                for x2, y2 in neighbours():
                    send(
                        at, at, tp_ss, t_rs.at[place],
                        (x2 * CORES + core, z * L + y2), has if s else None, True,
                    )

    def weights_on(s):
        for d, direction in enumerate((1, -1)):
            zs = z - direction * s
            nz = z + direction
            has = jnp.logical_and(zs >= 0, zs < Z)
            go = jnp.logical_and(has, jnp.logical_and(nz >= 0, nz < Z))
            block = jnp.clip(zs, 0, Z - 1)
            at = wg.at[rows(block, Dp)]
            if s:
                pl.when(has)(lambda: arrived(at, w_rs.at[block]))
            send(at, at, w_ss.at[d, s], w_rs.at[block], (r, jnp.clip(nz, 0, Z - 1) * L + y), go)

    texts_on(0)
    weights_on(0)
    loads[3].wait()

    def put_pool(at, value):
        pool[:, at:at + Db] = value

    by_half(pv[...].astype(F32), put_pool)
    loads[4].wait()
    loads[5].wait()
    eye = lax.broadcasted_iota(jnp.int32, (Db, Db), 0) == lax.broadcasted_iota(jnp.int32, (Db, Db), 1)
    line = jnp.broadcast_to(rmv[...].reshape(1, Db), (Db, Db))
    rmc[...] = jnp.sum(jnp.where(eye, line, 0.0), axis=1, keepdims=True)
    spans = (
        (pl.multiple_of(jnp.where(low, 0, Fw), 128), F2p - Fw),
        (pl.multiple_of(jnp.where(low, F2p - Fw, 0), 128), Fw),
    )

    def project(g):
        start, width = spans[g]
        lanes = pl.ds(start, width)
        for side in (1 - core, core):
            for o in range(1, X + 1):
                x2 = lax.rem(x + o, X)
                at = rows(x2 * CORES + side, L * T)
                part[at, lanes] = dot_nt(hid[at], wg[lanes])
                if side is not core:
                    send(part.at[at, lanes], pre.at[x2, :, lanes], pp_ss, pp_rs.at[x2, g], partner, bulk=True)

    def spread(g):
        start, width = spans[g]
        lanes = pl.ds(start, width)
        for o in range(1, X + 1):
            x2 = lax.rem(x + o, X)
            arrived(pre.at[x2, :, lanes], pp_rs.at[x2, g])
            summed[x2, :, lanes] = part[rows(x2 * CORES + core, L * T), lanes] + pre[x2, :, lanes]
            for k in range(L):
                y2 = lax.rem(y + 1 + k, L)
                if o == X and k == L - 1:
                    proj[x, y, :, lanes] = summed[x, rows(y, T), lanes]
                else:
                    send(
                        summed.at[x2, rows(y2, T), lanes], proj.at[x, y, :, lanes], p_ss,
                        p_rs.at[g], (x2 * CORES + core, z * L + y2), bulk=True,
                    )

    def gathered(g):
        start, width = spans[g]
        arrived(part.at[pl.ds(0, (X * L - 1) * T), pl.ds(start, width)], p_rs.at[g])

    def hidden_in():
        arrived(hid.at[pl.ds(0, (plane - 1 - crossing) * T)], hid_rs)

    for s in range(1, Z):
        texts_on(s)
        if s == 1:
            hidden_on()
        if s == Z - 1:
            spread(0)
        else:
            weights_on(s)
        relay(s - 1)
        if s == Z - 2:
            hidden_in()
            project(0)
            if E:
                send(hid, hid2, hf_ss, hf_rs, (r, nest * L + y), edge)
    weights_on(Z - 1)
    project(1)
    sent(part.at[pl.ds(0, X * L * T)], pp_ss)
    sent(part.at[pl.ds(0, (X * L - 1) * T)], p_ss)
    relay(Z - 1)
    spread(1)
    pairs_each = (X - 1) * (L - 1) * T
    sent(txa.at[pl.ds(0, Z * pairs_each)], td_ss)
    sent(txa.at[pl.ds(0, Z * (X + L - 2) * T)], tp_ss)
    gathered(0)
    gathered(1)
    for h in range(L):
        total = proj[0, h]
        for k in range(1, X):
            total = total + proj[k, h]
        mix[:, h * F2:(h + 1) * F2] = total[:, :F2]
    mixed = mix[...] + pool[...]
    length = jnp.sqrt(jnp.sum(mixed * mixed, axis=1, keepdims=True) + EPSILON)
    unit = mixed / length
    imgs[:T] = unit.astype(BF16)
    theirs = imgs.at[pl.ds(T, T)]
    send(imgs.at[pl.ds(0, T)], theirs, pair_ss.at[0], pair_rs.at[0], partner)
    scale = jnp.exp(jnp.full((1, 1), ls_ref[0], F32))
    bias = jnp.full((1, 1), bias_ref[0], F32)
    width = X * L * T

    def pairs(top, count, zs, blocks=1):
        images = imgs[top:top + count]
        texts = txa[pl.ds(pl.multiple_of(zs * width, width), blocks * width)]
        logits = scale * dot_nt(images, texts) + bias
        row_id = lax.broadcasted_iota(jnp.int32, logits.shape, 0) + top
        col_id = lax.broadcasted_iota(jnp.int32, logits.shape, 1) + (zs * width - own_slot * T)
        match = jnp.logical_and(row_id == col_id, row_id < T)
        u = jnp.where(match, -logits, logits)
        e = jnp.exp(-jnp.abs(u))
        loss = jnp.sum(jnp.maximum(u, 0.0) + jnp.log1p(e), axis=1, keepdims=True)
        sig = jnp.where(u >= 0, F32(1.0), e) / (1.0 + e)
        pg = (jnp.where(match, -sig, sig) / batch).astype(BF16)
        return loss, jnp.dot(pg, texts, preferred_element_type=F32)

    def total(top):
        loss, grads = pairs(top, T, 0, wide)
        if Z <= wide:
            return loss, grads

        def more(k, carry):
            loss, grads = pairs(top, T, k * wide, wide)
            return carry[0] + loss, carry[1] + grads

        return lax.fori_loop(1, Z // wide, more, (loss, grads))

    wide = max(w for w in (1, 2, 4) if Z % w == 0)
    arrived(txa.at[pl.ds(0, Z * pairs_each)], td_rs)
    loss_a, grads_a = total(0)
    arrived(theirs, pair_rs.at[0])
    loss_b, grads_b = total(T)
    ug_s[...] = scale * grads_b
    send(ug_s, ug_r, pair_ss.at[1], pair_rs.at[1], partner)
    arrived(ug_r, pair_rs.at[1])
    ug = scale * grads_a + ug_r[...]
    inner = jnp.sum(unit * ug, axis=1, keepdims=True)
    mg = ((ug - unit * inner) / length).astype(BF16)
    for h in range(L):
        mg_s[h, :, :F2] = mg[:, h * F2:(h + 1) * F2]
    others = [
        (lax.rem(x + ox, X), lax.rem(y + oy, L))
        for ox in reversed(range(X)) for oy in reversed(range(L)) if ox or oy
    ]
    everyone = others + [(x, y)]
    if E:
        for h in range(L):
            top = mg[:, h * F2 + (Z - 1) * Dp:h * F2 + Z * Dp]
            mgx_s[h] = jnp.where(low, top, mg[:, h * F2:h * F2 + Dp])
    mga[rows(q, T)] = mg_s[y]
    loss_local = jnp.sum(loss_a + loss_b, axis=0, keepdims=True)
    csb[c, :, Fb:Fb + 1] = loss_local
    def far_out():
        for x2, y2 in everyone:
            send(
                mgx_s.at[y2], mgx.at[rows(q, T)], mgx_ss, mgx_rs.at[q],
                (x2 * CORES + core, nest * L + y2), bulk=True,
            )

    def exchange(lanes, also=None):
        for x2, y2 in others:
            send(
                mg_s.at[y2, :, lanes], mga.at[rows(q, T), lanes], mg_ss, mg_rs.at[q],
                (x2 * CORES + core, z * L + y2), bulk=True,
            )
        send(mg_s.at[y, :, lanes], mga.at[rows(q, T), lanes], mg_ss, mg_rs.at[q], partner, bulk=True)
        if also is not None:
            also()
        for x2, y2 in others:
            source = (x2 * CORES + core) * L + y2
            at = mga.at[rows(source, T), lanes]
            arrived(at, mg_rs.at[source])
            send(at, at, mg_ss, mg_rs.at[source], partner, bulk=True)
        for x2, y2 in [(x, y)] + others:
            source = (x2 * CORES + 1 - core) * L + y2
            arrived(mga.at[rows(source, T), lanes], mg_rs.at[source])

    def exchanged(lanes):
        arrived(mga.at[pl.ds(0, (plane - 1) * T), lanes], mg_ss)

    every = pl.ds(0, F2p)
    if E:
        most = max(-(-(F2 - Dp) // 128) * 128, F2p - Dp // 128 * 128)
        needed = pl.ds(pl.multiple_of(jnp.where(low, 0, F2p - most), 128), most)
        pl.when(edge)(lambda: exchange(needed, far_out))
        pl.when(jnp.logical_not(edge))(lambda: exchange(every))
        finish.append(lambda: pl.when(edge)(lambda: exchanged(needed)))
        finish.append(lambda: pl.when(jnp.logical_not(edge))(lambda: exchanged(every)))
    else:
        exchange(every)
        finish.append(lambda: exchanged(every))
    if E:
        finish.append(lambda: pl.when(jnp.logical_or(edge, nearby))(
            lambda: arrived(mgx.at[pl.ds(0, X * L * T)], mgx_ss)
        ))

    turned[...] = mga[...].T

    def own_part(zd):
        gp[zd] = jnp.dot(turned[rows(zd, Dp)], hid[...], preferred_element_type=F32)

    def far_part():
        for x2, y2 in everyone:
            at = mgx.at[rows((x2 * CORES + core) * L + y2, T)]
            arrived(at, mgx_rs.at[(x2 * CORES + core) * L + y2])
            send(at, at, mgx_ss, mgx_rs.at[(x2 * CORES + core) * L + y2], partner, bulk=True)
        arrived(hid2, hf_rs)
        for x2, y2 in everyone:
            source = (x2 * CORES + 1 - core) * L + y2
            arrived(mgx.at[rows(source, T)], mgx_rs.at[source])
        gp[theirs_far] = gp[theirs_far] + jnp.dot(mgx[...].T, hid2[...], preferred_element_type=F32)

    def pieces(tau, d):
        place = z if d == 0 else Z - 1 - z
        far = Z - 1 if d == 0 else 0
        i = tau - 2 * jnp.maximum(place - E, 0) + jnp.where(place == 0, K * E, 0)
        zd = jnp.clip(i, 0, Z * K - 1) // K
        k = jnp.clip(i, 0, Z * K - 1) % K
        zd = Z - 1 - zd if d == 0 else zd
        beyond = zd > z if d == 0 else zd < z
        ready = jnp.logical_and(i >= 0, i < Z * K)
        opens = jnp.logical_or(place == 0, jnp.logical_and(place == E, zd == far))
        return zd, k, jnp.logical_and(ready, beyond), jnp.logical_and(ready, zd == z), opens, place

    def step(tau, held):
        for d in range(2):
            zd, k, passing, ending, opens, place = pieces(tau, d)
            cut = rows(k, Dc)
            at = gz.at[d, zd, cut]
            copy = pltpu.make_async_remote_copy(
                src_ref=gz_s.at[zd, cut], dst_ref=at, send_sem=g_ss, recv_sem=g_rs.at[zd + 1 - d, k],
                device_id=(r, jnp.clip(z + (1 if d == 0 else -1), 0, Z - 1) * L + y), device_id_type=MESH,
            )

            def first():
                gz_s[zd, cut] = gp[zd, cut].astype(BF16)
                copy.start()

            def onward():
                arrived(at, g_rs.at[zd + 1 - d, k])
                gz_s[zd, cut] = (gp[zd, cut] + at[...].astype(F32)).astype(BF16)
                copy.start()

            def last():
                arrived(at, g_rs.at[zd + 1 - d, k])
                gp[zd, cut] = gp[zd, cut] + at[...].astype(F32)

            passing = jnp.logical_and(passing, held)
            ending = jnp.logical_and(jnp.logical_and(ending, held), place > 0)
            pl.when(jnp.logical_and(passing, opens))(first)
            pl.when(jnp.logical_and(passing, jnp.logical_not(opens)))(onward)
            pl.when(ending)(last)

    def early(tau, _):
        step(tau, edge)
        return _

    def later(tau, _):
        step(tau, jnp.logical_or(jnp.logical_not(edge), tau >= head))
        return _

    steps_g = max((Z - 1) * K + 1 - 2 * E, K - 1 + 2 * (Z - 1 - E)) + 1
    head = 2

    def order(k):
        return jnp.where(low, Z - 1 - k, k)

    if E:
        own_part(order(1))
        lax.fori_loop(0, head, early, 0)
        pl.when(jnp.logical_not(edge))(lambda: own_part(order(0)))
        for k in range(2, Z):
            own_part(order(k))
        finish.append(lambda: pl.when(edge)(lambda: arrived(gz_s.at[pl.ds(0, Z - 2)], g_ss)))
        finish.append(lambda: pl.when(jnp.logical_not(edge))(lambda: arrived(gz_s.at[pl.ds(0, Z - 1)], g_ss)))
    else:
        for k in range(Z):
            own_part(order(k))
        sent(gz_s.at[pl.ds(0, Z - 1)], g_ss)
    lax.fori_loop(0, head, later, 0)
    if E:
        pl.when(nearby)(far_part)
    lax.fori_loop(head, steps_g, later, 0)
    g = gp[z][:Db]

    def across_cols(box, ss, rs):
        for o in range(1, C):
            send(box.at[c], box.at[c], ss, rs, (r, lax.rem(c + o, C)), bulk=True)
        sent(box.at[pl.ds(0, C - 1)], ss)

    def across_rows(box, ss, rs, also=lambda: None):
        for o in range(1, R):
            send(box.at[r], box.at[r], ss, rs, (lax.rem(r + o, R), c), bulk=True)
        sent(box.at[pl.ds(0, R - 1)], ss)
        also()
        arrived(box.at[pl.ds(0, R - 1)], rs)

    square = g * g
    sq = square + FLOOR_VALUE
    rsb[r] = jnp.sum(jnp.where(eye, jnp.sum(sq, axis=1, keepdims=True), 0.0), axis=0, keepdims=True)
    csb[c, :, :Fb] = jnp.sum(sq, axis=0, keepdims=True)
    across_rows(rsb, row_ss, row_rs, lambda: across_cols(csb, col_ss, col_rs))
    row_sum = jnp.broadcast_to(sum(rsb[k] for k in range(R)), (Db, Db))
    row_sum = jnp.sum(jnp.where(eye, row_sum, 0.0), axis=1, keepdims=True)
    new_row = DECAY_RATE * rmc[...] + (1.0 - DECAY_RATE) * row_sum / (R * Fb)
    qcb[c] = jnp.sum(square / new_row, axis=0, keepdims=True)
    across_cols(qcb, qc_ss, qc_rs)
    nr_ref[...] = jnp.sum(jnp.where(eye, new_row, 0.0), axis=0)
    arrived(csb.at[pl.ds(0, C - 1)], col_rs)
    col_sum = sum(csb[k] for k in range(C))
    new_col = DECAY_RATE * cmv[...].reshape(1, Fb) + (1.0 - DECAY_RATE) * col_sum[:, :Fb] / (C * Db)
    nc_ref[...] = new_col[0]
    upd_ref[...] = g / jnp.sqrt(new_row * new_col)
    for i, (src, dst) in enumerate(((upd_ref, upd_out), (nr_ref, nr_out), (nc_ref, nc_out))):
        store = pltpu.make_async_copy(src, dst, ld.at[6 + i])
        store.start()
        finish.append(store.wait)
    arrived(qcb.at[pl.ds(0, C - 1)], qc_rs)
    part_sum = jnp.sum(sum(qcb[k] for k in range(C)) / new_col, axis=1, keepdims=True)
    lane = lax.broadcasted_iota(jnp.int32, (1, 128), 1)
    srb[r] = jnp.where(lane == 0, part_sum, col_sum[:, Fb:Fb + 1])
    across_rows(srb, sr_ss, sr_rs)
    totals = sum(srb[k] for k in range(R))
    rms = jnp.sqrt(totals / (C * Db * R * Fb))
    end_v[...] = jnp.where(lane == 0, jnp.maximum(1.0, rms / CLIP_LEVEL), totals / batch)
    store = pltpu.make_async_copy(end_v, end_ref, ld.at[9])
    store.start()
    finish.append(store.wait)
    for wait in finish:
        wait()


def divide(raw_ref, row_ref, col_ref, end_ref, upd_ref, nr_ref, nc_ref, loss_ref):
    upd_ref[...] = raw_ref[...] / end_ref[:, 0:1]
    nr_ref[...] = row_ref[...]
    nc_ref[...] = col_ref[...]
    lane = lax.broadcasted_iota(jnp.int32, (1, 128), 1)
    loss_ref[0] = jnp.sum(jnp.where(lane == 1, end_ref[...], 0.0))


def per_device(pooled, hidden, text, weight, row_moment, col_moment, log_scale, bias):
    R, C = lax.axis_size("row"), lax.axis_size("col")
    L, X, Z = LOW, R // CORES, C // LOW
    T, D = pooled.shape
    Db, Fb = weight.shape
    Dp = -(-Db // 16) * 16
    F2 = Z * Dp
    plane = R * L
    texts = X * C * T

    K = 3 if Dp % 48 == 0 else 1
    E = 1 if Z == 4 or Z > 5 else 0
    F2p = -(-F2 // 128) * 128
    Fw = max(-(-Dp // 128) * 128, F2p - (F2 - Dp) // 128 * 128)
    sizes = (R, C, X, Z, T, Db, Dp, Fb, K, E, F2, F2p, Fw)
    vmem = pl.BlockSpec(memory_space=pltpu.VMEM)
    smem = pl.BlockSpec(memory_space=pltpu.SMEM)
    dma = lambda *s: pltpu.SemaphoreType.DMA(s)
    one = pltpu.SemaphoreType.DMA
    raw = pl.pallas_call(
        functools.partial(kernel, sizes),
        out_shape=(
            jax.ShapeDtypeStruct((Db, Fb), F32),
            jax.ShapeDtypeStruct((Db,), F32),
            jax.ShapeDtypeStruct((Fb,), F32),
            jax.ShapeDtypeStruct((1, 128), F32),
        ),
        in_specs=[pl.BlockSpec(memory_space=pl.ANY)] * 6 + [smem] * 2,
        out_specs=(pl.BlockSpec(memory_space=pl.ANY),) * 4,
        scratch_shapes=[
            pltpu.VMEM((T, R * Fb), BF16),
            pltpu.VMEM((Db, Fb), F32),
            pltpu.VMEM((T, D), BF16),
            pltpu.VMEM((T, D), BF16),
            pltpu.VMEM((Db,), F32),
            pltpu.VMEM((Fb,), F32),
            pltpu.VMEM((R, T, Fb), BF16),
            pltpu.VMEM((T, L * F2), F32),
            pltpu.VMEM((Db, 1), F32),
            pltpu.VMEM((plane * T, Fb), BF16),
            pltpu.VMEM((F2p, Fb), BF16),
            pltpu.VMEM((texts, L * F2), BF16),
            pltpu.VMEM((plane * T, F2p), F32),
            pltpu.VMEM((X, L * T, F2p), F32),
            pltpu.VMEM((X, L * T, F2p), F32),
            pltpu.VMEM((X, L, T, F2p), F32),
            pltpu.VMEM((T, L * F2), F32),
            pltpu.VMEM((2 * T, L * F2), BF16),
            pltpu.VMEM((T, L * F2), F32),
            pltpu.VMEM((T, L * F2), F32),
            pltpu.VMEM((L, T, F2p), BF16),
            pltpu.VMEM((plane * T, F2p), BF16),
            pltpu.VMEM((F2p, plane * T), BF16),
            pltpu.VMEM((Z, Dp, Fb), F32),
            pltpu.VMEM((Z, Dp, Fb), BF16),
            pltpu.VMEM((2, Z, Dp, Fb), BF16),
            pltpu.VMEM((Db, Fb), F32),
            pltpu.VMEM((Db,), F32),
            pltpu.VMEM((Fb,), F32),
            pltpu.VMEM((1, 128), F32),
            pltpu.VMEM((R, 1, Db), F32),
            pltpu.VMEM((C, 1, Fb + 1), F32),
            pltpu.VMEM((C, 1, Fb), F32),
            pltpu.VMEM((R, 1, 128), F32),
            pltpu.VMEM((plane * T, Fb), BF16),
            pltpu.VMEM((L, T, Dp), BF16),
            pltpu.VMEM((plane * T, Dp), BF16),
            dma(10),
            one, one, one, dma(2, Z), dma(Z), dma(2, Z), one, dma(X * C), one, one,
            one, dma(X, 2), one, dma(2), dma(2), dma(2),
            one, dma(plane), one, dma(Z + 1, K), one, one, one, one,
            one, one, one, one, one, one, one, dma(plane),
        ],
        compiler_params=pltpu.CompilerParams(
            has_side_effects=True, collective_id=0, vmem_limit_bytes=60 * 1024 * 1024
        ),
    )(
        hidden, weight, pooled, text, row_moment, col_moment, log_scale[None], bias[None],
    )
    upd, nr, nc, loss = pl.pallas_call(
        divide,
        out_shape=(
            jax.ShapeDtypeStruct((Db, Fb), F32),
            jax.ShapeDtypeStruct((Db,), F32),
            jax.ShapeDtypeStruct((Fb,), F32),
            jax.ShapeDtypeStruct((1,), F32),
        ),
        in_specs=[vmem] * 4,
        out_specs=(vmem,) * 3 + (smem,),
    )(*raw)
    return upd, nr, nc, loss[0]


def solution(mesh):
    return jax.shard_map(
        per_device,
        mesh=mesh,
        in_specs=(
            P(("row", "col"), None),
            P(("row", "col"), None),
            P(("row", "col"), None),
            P("col", "row"),
            P("col"),
            P("row"),
            P(),
            P(),
        ),
        out_specs=(P("col", "row"), P("col"), P("row"), P()),
        check_vma=False,
    )
```
